512 devices in a mesh: members: 2 (over y), band: 32 (over z, core), head: 8 (over x).
Axes of the slice: x: 8, y: 2, z: 16, core: 2. Of those that a mesh axis runs over, the one named last changes fastest.
The devices are a block of a 8x8x16 slice.
Arguments:
- grid_feats: bfloat16 [32768, 1024], P(('members', 'band')), parts along dimension 0, may hold values from -6 to 6
- mesh_feats: bfloat16 [32768, 1024], P(('members', 'band')), parts along dimension 0, may hold values from -6 to 6
- enc_in: bfloat16 [3, 1024, 1024], P(None, 'band', 'head'), may hold values from -0.19921875 to 0.19921875
- enc_out: bfloat16 [1024, 1024], P('head', 'band'), may hold values from -0.1875 to 0.1875
- proc_in: bfloat16 [3, 1024, 1024], P(None, 'band', 'head'), may hold values from -0.19921875 to 0.19921875
- proc_out: bfloat16 [1024, 1024], P('head', 'band'), may hold values from -0.1875 to 0.1875
- ff_up: bfloat16 [1024, 4096], P('band', 'head'), may hold values from -0.1875 to 0.1875
- ff_down: bfloat16 [4096, 1024], P('head', 'band'), may hold values from -0.09375 to 0.09375
- dec_in: bfloat16 [3, 1024, 1024], P(None, 'band', 'head'), may hold values from -0.19921875 to 0.19921875
- dec_out: bfloat16 [1024, 1024], P('head', 'band'), may hold values from -0.1875 to 0.1875
- enc_list: int32 [128, 8], replicated, may hold values from 0 to 127, as said below
- enc_count: int32 [128], replicated, may hold values from 1 to 8
- dec_list: int32 [128, 8], replicated, may hold values from 0 to 127, as said below
- dec_count: int32 [128], replicated, may hold values from 1 to 8
- window_ids: int32 [16384], replicated, may hold values from 0 to 20, never falling along the last dimension, each value on 1 to 1536 neighbouring positions
Outputs:
- grid_out: bfloat16 [32768, 1024], P(('members', 'band', 'head')), parts along dimension 0
The draws below stay inside these ranges and needn't reach their ends.
There are 2 independent parts, one for each index of `members`. The reference program is written for one: setup_inputs(seed, part) draws one part's arguments, and reference() takes and returns one part's arrays. A program takes and returns all parts, laid end to end along the dimension named above; an argument that names none is the same for every part. Nothing has to cross between parts.
Inputs may be any that keep to these rules, and one draw needn't show every extreme that they name: `enc_list`: each row holds distinct block numbers. Every block listed for mesh block m lies in the band of 512 grid points with the same band number as m's band of 512 nodes, or in the band just before or just after it. Only the first enc_count[m] slots of row m of enc_list are used. `dec_list`: each row holds distinct block numbers. Every block listed for grid block g lies in the band of 512 mesh nodes with the same band number as g's band of 512 grid points, or in the band just before or just after it. Only the first dec_count[g] slots of row g of dec_list are used. `window_ids`: never falls along the nodes; each window holds at most 1536 consecutive nodes.
All inputs are finite; a program needn't handle non-finite values.
Results may differ from the reference program's by a relative error of at most 0.02.
Values may be sent and summed in bfloat16 or wider, within the bound.
A program may use at most 64 MiB of HBM per device.

```python
import math
import jax
import jax.numpy as jnp
import numpy as np
from jax import lax

D = 1024
HEADS = 16
FF = 4096
HD = 64
BLOCK = 128
LIST = 8
WINDOW = 1536
GRID_DEV = 512
MESH_DEV = 512
GRID = 16384
MESH = 16384
WINDOWS = 21
N_HEAD = 8


def block_choice(key, query_blocks, query_per_band, cand_per_band, cand_total):
    band_of = jnp.arange(query_blocks, dtype=jnp.int32) // query_per_band
    offsets = jnp.arange(3 * cand_per_band, dtype=jnp.int32)
    candidates = (band_of[:, None] - 1) * cand_per_band + offsets[None, :]
    usable = (candidates >= 0) & (candidates < cand_total)
    scores = jax.random.randint(key, (query_blocks, 3 * cand_per_band), 0, 1 << 20, dtype=jnp.int32)
    scores = scores * (3 * cand_per_band) + offsets[None, :]
    scores = jnp.where(usable, scores, (1 << 30) + offsets[None, :])
    order = jnp.argsort(scores, axis=1, stable=True)
    picked = jnp.take_along_axis(candidates, order[:, :LIST], axis=1)
    return picked.astype(jnp.int32)


def draw_enc_list(key, part):
    return block_choice(jax.random.fold_in(key, 11), MESH // BLOCK, MESH_DEV // BLOCK, GRID_DEV // BLOCK, GRID // BLOCK)


def draw_dec_list(key, part):
    return block_choice(jax.random.fold_in(key, 23), GRID // BLOCK, GRID_DEV // BLOCK, MESH_DEV // BLOCK, MESH // BLOCK)


def projection_base(key):
    return jax.random.truncated_normal(key, -6.0, 6.0, (3, D, D), jnp.float32) * D ** (-0.5)


def state_base(key, count):
    return jax.random.truncated_normal(key, -6.0, 6.0, (count, D), jnp.float32)


def draw_enc_in(key, part):
    base = projection_base(jax.random.fold_in(key, 31))
    return base.astype(jnp.bfloat16)


def draw_proc_in(key, part):
    base = projection_base(jax.random.fold_in(key, 37))
    return base.astype(jnp.bfloat16)


def draw_dec_in(key, part):
    base = projection_base(jax.random.fold_in(key, 41))
    return base.astype(jnp.bfloat16)


def draw_grid_feats(key, part):
    base = state_base(jax.random.fold_in(key, 43), GRID)
    return base.astype(jnp.bfloat16)


def draw_mesh_feats(key, part):
    base = state_base(jax.random.fold_in(key, 53), MESH)
    return base.astype(jnp.bfloat16)


def plant(array, stream_key, low, largest):
    extent = array.shape
    place = [jax.random.randint(jax.random.fold_in(stream_key, axis), (), 0, extent[axis]) for axis in range(len(extent))]
    array = array.at[tuple(place)].set(low)
    longest = extent.index(max(extent))
    place[longest] = (place[longest] + 1) % extent[longest]
    return array.at[tuple(place)].set(largest)


def levels(rng, dims, pieces, smallest, high):
    gain = 1.0
    for position, shards_of in pieces:
        steps = jax.random.uniform(jax.random.fold_in(jax.random.fold_in(rng, 6), position), (shards_of,), jnp.float32, smallest / len(pieces), high / len(pieces))
        gain = gain * jnp.repeat(jnp.exp(steps), dims[position] // shards_of).reshape((-1,) + (1,) * (len(dims) - 1 - position))
    return gain


def profile(number_of, total, limit, slope):
    portions = [(1 << 20) // math.isqrt(rank ** slope) + 1 for rank in range(2, number_of + 1)]
    surplus, given = total - limit - (number_of - 1), [1] * (number_of - 1)
    while surplus > 0:
        free = [i for i in range(number_of - 1) if given[i] < limit]
        whole, budget = sum([portions[i] for i in free]), surplus
        for i in free:
            more = min(limit - given[i], max(1, budget * portions[i] // whole), surplus)
            given[i] = given[i] + more
            surplus = surplus - more
    return np.array([limit] + given)


def uneven_parts(stream_key, amount, total, reach, lean):
    if amount == 2:
        one = jax.random.randint(stream_key, (), max(1, total - reach), min(reach, total - 1) + 1)
        return jnp.stack([one, total - one])
    tallies = jnp.asarray(profile(amount, total, reach, lean), jnp.int32)
    couples = (amount - 1) // 2
    giver, taker = tallies[1:1 + 2 * couples:2], tallies[2:2 + 2 * couples:2]
    room = jnp.minimum(giver - 1, reach - taker)
    passed = jax.random.randint(jax.random.fold_in(stream_key, 1), (couples,), 0, 1 << 20) % (room + 1)
    tallies = tallies.at[1:1 + 2 * couples:2].set(giver - passed).at[2:2 + 2 * couples:2].set(taker + passed)
    return tallies[jax.random.permutation(jax.random.fold_in(stream_key, 2), amount)]


def normal_values(key, dims, width, limit, split=(), kind=jnp.bfloat16):
    values = jax.random.normal(key, dims, jnp.float32) * width
    if len(split) > 0:
        values = levels(key, dims, split, -0.22, 0.18) * values
    return jnp.clip(values, min=-limit, max=limit).astype(kind)


def setup_inputs(seed: int = 0, part: int = 0) -> dict:
    key_of = jax.random.split(jax.random.key(seed), 16)
    part_keys = jax.random.split(jax.random.fold_in(key_of[15], part), 16)
    grid_feats = draw_grid_feats(jax.random.fold_in(jax.random.fold_in(key_of[15], part), 71), part)
    mesh_feats = draw_mesh_feats(jax.random.fold_in(jax.random.fold_in(key_of[15], part), 71), part)
    enc_in = draw_enc_in(jax.random.fold_in(key_of[15], 71), part)
    enc_out = normal_values(key_of[3], (D, D), D ** -0.5, 0.1875, ((0, 8), (1, 32)))
    proc_in = draw_proc_in(jax.random.fold_in(key_of[15], 71), part)
    proc_out = normal_values(key_of[5], (D, D), D ** -0.5, 0.1875, ((0, 8), (1, 32)))
    ff_up = normal_values(key_of[6], (D, FF), D ** -0.5, 0.1875, ((0, 32), (1, 8)))
    ff_down = normal_values(key_of[7], (FF, D), FF ** -0.5, 0.09375, ((0, 8), (1, 32)))
    dec_in = draw_dec_in(jax.random.fold_in(key_of[15], 71), part)
    dec_out = normal_values(key_of[9], (D, D), D ** -0.5, 0.1875, ((0, 8), (1, 32)))
    enc_list = draw_enc_list(jax.random.fold_in(key_of[15], 71), part)
    enc_count = plant(jax.random.randint(key_of[11], (MESH // BLOCK,), 1, LIST + 1), jax.random.fold_in(key_of[11], 1), 1, LIST).astype(jnp.int32)
    dec_list = draw_dec_list(jax.random.fold_in(key_of[15], 71), part)
    dec_count = plant(jax.random.randint(key_of[13], (GRID // BLOCK,), 1, LIST + 1), jax.random.fold_in(key_of[13], 1), 1, LIST).astype(jnp.int32)
    window_ids = jnp.searchsorted(jnp.cumsum(uneven_parts(key_of[14], WINDOWS, MESH, WINDOW, 0)), jnp.arange(MESH), side="right").astype(jnp.int32)
    return {"grid_feats": grid_feats, "mesh_feats": mesh_feats, "enc_in": enc_in, "enc_out": enc_out, "proc_in": proc_in, "proc_out": proc_out, "ff_up": ff_up, "ff_down": ff_down, "dec_in": dec_in, "dec_out": dec_out, "enc_list": enc_list, "enc_count": enc_count, "dec_list": dec_list, "dec_count": dec_count, "window_ids": window_ids}


EPSILON = 1e-05
NEGATIVE = -1e+30
HIGHEST = lax.Precision.HIGHEST

def normed(source):
    values_f = source.astype(jnp.float32)
    centred = values_f - lax.optimization_barrier(jnp.mean(values_f, axis=-1, keepdims=True))
    variance = lax.optimization_barrier(jnp.mean(centred * centred, axis=-1, keepdims=True))
    return (centred * lax.rsqrt(variance + EPSILON)).astype(jnp.bfloat16)

def project(source, weight):
    return jnp.dot(source, weight, preferred_element_type=jnp.float32).astype(jnp.bfloat16)

def group_sum(source, weight):
    inner = source.shape[1] // N_HEAD
    total = jnp.zeros((source.shape[0], weight.shape[1]), jnp.float32)
    for group in range(N_HEAD):
        part_sum = jnp.dot(source[:, group * inner:(group + 1) * inner], weight[group * inner:(group + 1) * inner], preferred_element_type=jnp.float32)
        rounded = lax.optimization_barrier(part_sum.astype(jnp.bfloat16))
        total = total + rounded.astype(jnp.float32)
    return total

def split_heads(rows):
    return rows.astype(jnp.float32).reshape(rows.shape[0], HEADS, HD)

def softmax_parts(queries, key_rows, allowed):
    scores = jnp.einsum('qhd,khd->hqk', split_heads(queries), split_heads(key_rows), precision=HIGHEST) * HD ** (-0.5)
    scores = jnp.where(allowed[None], scores, NEGATIVE)
    maxima = lax.optimization_barrier(jnp.max(scores, axis=-1, keepdims=True))
    expo = jnp.exp(scores - maxima) * allowed[None].astype(jnp.float32)
    return (expo, lax.optimization_barrier(jnp.sum(expo, axis=-1, keepdims=True)))

def listed_attention(queries, key_rows, value_rows, lists, counts, rounded_weights):
    key_blocks = key_rows.reshape(key_rows.shape[0] // BLOCK, BLOCK, D)
    value_blocks = value_rows.reshape(value_rows.shape[0] // BLOCK, BLOCK, D)

    def one_block(index):
        listed = lists[index]
        live = jnp.arange(LIST, dtype=jnp.int32) < counts[index]
        block_keys = key_blocks[listed].reshape(LIST * BLOCK, D)
        block_values = value_blocks[listed].reshape(LIST * BLOCK, D)
        allowed = jnp.repeat(live, BLOCK)[None, :]
        block_queries = lax.dynamic_slice_in_dim(queries, index * BLOCK, BLOCK, 0)
        expo, totals = softmax_parts(block_queries, block_keys, allowed)
        if rounded_weights:
            weights = (expo / totals).astype(jnp.bfloat16).astype(jnp.float32)
            mixed = jnp.einsum('hqk,khd->qhd', weights, split_heads(block_values), precision=HIGHEST)
        else:
            mixed = jnp.einsum('hqk,khd->qhd', expo, split_heads(block_values), precision=HIGHEST)
            mixed = mixed / jnp.transpose(totals, (1, 0, 2))
        return mixed.reshape(BLOCK, D).astype(jnp.bfloat16)
    blocks = lax.map(one_block, jnp.arange(queries.shape[0] // BLOCK, dtype=jnp.int32))
    return blocks.reshape(queries.shape[0], D)

def window_attention(queries, key_rows, value_rows, window_ids):
    padded_keys = jnp.pad(key_rows, ((WINDOW, WINDOW), (0, 0)))
    padded_values = jnp.pad(value_rows, ((WINDOW, WINDOW), (0, 0)))
    padded_ids = jnp.pad(window_ids, (WINDOW, WINDOW), constant_values=-1)

    def one_block(index):
        start = index * BLOCK
        block_queries = lax.dynamic_slice_in_dim(queries, start, BLOCK, 0)
        block_keys = lax.dynamic_slice_in_dim(padded_keys, start, BLOCK + 2 * WINDOW, 0)
        block_values = lax.dynamic_slice_in_dim(padded_values, start, BLOCK + 2 * WINDOW, 0)
        key_ids = lax.dynamic_slice_in_dim(padded_ids, start, BLOCK + 2 * WINDOW, 0)
        query_ids = lax.dynamic_slice_in_dim(window_ids, start, BLOCK, 0)
        allowed = query_ids[:, None] == key_ids[None, :]
        expo, totals = softmax_parts(block_queries, block_keys, allowed)
        weights = (expo / totals).astype(jnp.bfloat16).astype(jnp.float32)
        mixed = jnp.einsum('hqk,khd->qhd', weights, split_heads(block_values), precision=HIGHEST)
        return mixed.reshape(BLOCK, D).astype(jnp.bfloat16)
    blocks = lax.map(one_block, jnp.arange(queries.shape[0] // BLOCK, dtype=jnp.int32))
    return blocks.reshape(queries.shape[0], D)

def reference(grid_feats, mesh_feats, enc_in, enc_out, proc_in, proc_out, ff_up, ff_down, dec_in, dec_out, enc_list, enc_count, dec_list, dec_count, window_ids):
    grid_norm = normed(grid_feats)
    mesh_norm = normed(mesh_feats)
    enc_q = project(mesh_norm, enc_in[0])
    enc_k = project(grid_norm, enc_in[1])
    enc_v = project(grid_norm, enc_in[2])
    enc_attn = listed_attention(enc_q, enc_k, enc_v, enc_list, enc_count, False)
    mesh_state = mesh_feats.astype(jnp.float32) + group_sum(enc_attn, enc_out)
    proc_norm = normed(mesh_state)
    proc_q = project(proc_norm, proc_in[0])
    proc_k = project(proc_norm, proc_in[1])
    proc_v = project(proc_norm, proc_in[2])
    proc_attn = window_attention(proc_q, proc_k, proc_v, window_ids)
    mesh_mid = mesh_state + group_sum(proc_attn, proc_out)
    hidden = jax.nn.gelu(jnp.dot(normed(mesh_mid), ff_up, preferred_element_type=jnp.float32), approximate=False).astype(jnp.bfloat16)
    mesh_final = mesh_mid + group_sum(hidden, ff_down)
    final_norm = normed(mesh_final)
    dec_q = project(grid_norm, dec_in[0])
    dec_k = project(final_norm, dec_in[1])
    dec_v = project(final_norm, dec_in[2])
    dec_attn = listed_attention(dec_q, dec_k, dec_v, dec_list, dec_count, True)
    return (grid_feats.astype(jnp.float32) + group_sum(dec_attn, dec_out)).astype(jnp.bfloat16)
```

```python
import functools

import jax
import jax.numpy as jnp
from jax import lax
from jax.experimental import pallas as pl
from jax.experimental.pallas import tpu as pltpu
from jax.sharding import PartitionSpec as P

HD = 64
BLOCK = 128
WINDOW = 1536
REACH = 3
EPSILON = 1e-05
NEGATIVE = -1e30
SCALE = HD ** (-0.5) * 1.4426950408889634
MESH_ID = pl.DeviceIdType.MESH


def contract_rows(left, right):
    return lax.dot_general(left, right, (((1,), (1,)), ((), ())), preferred_element_type=jnp.float32)


def normed(values):
    centred = values - jnp.mean(values, axis=-1, keepdims=True)
    variance = jnp.mean(centred * centred, axis=-1, keepdims=True)
    return (centred * lax.rsqrt(variance + EPSILON)).astype(jnp.bfloat16)


def kernel(
    nb,
    nh,
    grid_ref,
    mesh_ref,
    w_ref,
    enc_bias,
    dec_bias,
    key_ids,
    query_ids,
    out_ref,
    wall,
    x,
    gn,
    q,
    attn,
    hidden,
    p,
    slots,
    eslab,
    wslab,
    dslab,
    state,
    zs,
    zr,
    ps,
    pr,
    rss,
    rsr,
    ags,
    agr,
    hs,
    hr,
):
    b = lax.axis_index("band")
    h = lax.axis_index("head")
    rows, depth = grid_ref.shape
    width = q.shape[1]
    ff = hidden.shape[1]
    share = rows // nh
    half_cols = depth // 2
    wrows = w_ref.shape[0]
    nz = nb // 2
    odd = lax.rem(b, 2)
    partner = b + 1 - 2 * odd
    stages = (
        (0, 4 * width),
        (4 * width, 8 * width),
        (8 * width, 8 * width + 2 * ff),
        (8 * width + 2 * ff, 12 * width + 2 * ff),
    )

    def band(offset):
        return lax.rem(b + (offset + nb), nb)

    def head(offset):
        return lax.rem(h + (offset + nh), nh)

    def copy(src, dst, send_sem, recv_sem, **where):
        return pltpu.make_async_remote_copy(
            src_ref=src,
            dst_ref=dst,
            send_sem=send_sem,
            recv_sem=recv_sem,
            device_id={"band": where.get("band", b), "head": where.get("head", h)},
            device_id_type=MESH_ID,
        )

    sent = []

    barrier = pltpu.get_barrier_semaphore()
    peers = [{"band": band(o), "head": h} for o in (1, -1, 2, -2, 3, -3)]
    peers += [{"band": b, "head": head(o)} for o in (1, -1)]
    for peer in peers:
        pl.semaphore_signal(barrier, inc=1, device_id=peer, device_id_type=MESH_ID)
    pl.semaphore_wait(barrier, len(peers))

    right_steps = nz // 2
    left_steps = nz - 1 - right_steps

    def block(index, stage):
        low, high = stages[stage]
        return wall.at[pl.ds(pl.multiple_of(index * wrows, wrows), wrows), low:high]

    def own(stage):
        low, high = stages[stage]
        return w_ref.at[:, low:high]

    def zcopy(stage, way, step):
        index = band(2 * step if way else -2 * step)
        src = block(index, stage) if step else own(stage)
        return copy(
            src,
            block(index, stage),
            zs.at[stage, way, step],
            zr.at[stage, way, step],
            band=band(-2 if way else 2),
        )

    def pcopy(stage, k):
        index = band(2 * k)
        src = block(index, stage) if k else own(stage)
        return copy(src, block(index, stage), ps.at[stage, k], pr.at[stage, k], band=partner)

    def begin(one):
        one.start()
        sent.append(one)

    def zstart(stage):
        begin(zcopy(stage, 0, 0))
        if left_steps:
            begin(zcopy(stage, 1, 0))
        begin(pcopy(stage, 0))
        low, high = stages[stage]
        wall[pl.ds(pl.multiple_of(b * wrows, wrows), wrows), low:high] = w_ref[:, low:high]

    def zstep(stage, step):
        if step > right_steps:
            return
        zcopy(stage, 0, step - 1).wait_recv()
        if step < right_steps:
            begin(zcopy(stage, 0, step))
        begin(pcopy(stage, nz - step))
        if step - 1 < left_steps:
            zcopy(stage, 1, step - 1).wait_recv()
            if step < left_steps:
                begin(zcopy(stage, 1, step))
            begin(pcopy(stage, step))

    def zfinish(stage):
        for k in range(nz):
            pcopy(stage, k).wait_recv()

    longer = nh // 2
    shorter = nh - 1 - longer
    flows = ((1, 0, longer), (-1, 1, longer), (1, 1, shorter), (-1, 0, shorter))
    base = (0, longer, 2 * longer, 2 * longer + shorter)

    def share_rows(chunk):
        return pl.ds(pl.multiple_of(chunk * share, share), share)

    def half_of(half):
        return slice(half * half_cols, (half + 1) * half_cols)

    def rcopy(stage, flow, step):
        way, half, hops = flows[flow]
        slot = base[flow] + step
        return copy(
            p.at[share_rows(head(way * (hops - step))), half_of(half)],
            slots.at[slot],
            rss.at[stage, slot],
            rsr.at[stage, slot],
            head=head(way),
        )

    def acopy(stage, flow, step):
        way, half, hops = flows[flow]
        slot = base[flow] + step
        view = x.at[share_rows(head(-way * step)), half_of(half)]
        return copy(view, view, ags.at[stage, slot], agr.at[stage, slot], head=head(way))

    def summed(stage, next_stage):
        for step in range(longer):
            for flow, (way, half, hops) in enumerate(flows):
                if step < hops:
                    if step:
                        rcopy(stage, flow, step - 1).wait_recv()
                        where = share_rows(head(way * (hops - step)))
                        p[where, half_of(half)] = (
                            p[where, half_of(half)].astype(jnp.float32)
                            + slots[base[flow] + step - 1].astype(jnp.float32)
                        ).astype(jnp.bfloat16)
                    rcopy(stage, flow, step).start()
            if next_stage is not None:
                zstep(next_stage, step + 1)
        halves = [p[share_rows(h), half_of(half)].astype(jnp.float32) for half in range(2)]
        for flow, (way, half, hops) in enumerate(flows):
            rcopy(stage, flow, hops - 1).wait_recv()
            halves[half] = halves[half] + slots[base[flow] + hops - 1].astype(jnp.float32)
        for flow, (way, half, hops) in enumerate(flows):
            for step in range(hops):
                rcopy(stage, flow, step).wait_send()
        return jnp.concatenate(halves, axis=1)

    def gathered(stage, next_stage):
        for step in range(longer):
            for flow, (way, half, hops) in enumerate(flows):
                if step < hops:
                    if step:
                        acopy(stage, flow, step - 1).wait_recv()
                    acopy(stage, flow, step).start()
            zstep(next_stage, longer + step + 1)
        for flow, (way, half, hops) in enumerate(flows):
            acopy(stage, flow, hops - 1).wait_recv()
        for flow, (way, half, hops) in enumerate(flows):
            for step in range(hops):
                acopy(stage, flow, step).wait_send()
        for step in range(2 * longer + 1, right_steps + 1):
            zstep(next_stage, step)
        zfinish(next_stage)

    tile = min(256, rows)
    tiles = rows // tile

    def tile_rows(index, offset=0):
        return pl.ds(pl.multiple_of(offset + index * tile, tile), tile)

    def for_tiles(body):
        @pl.loop(0, tiles)
        def _(index):
            body(index)

    def norm_rows(src, dst):
        piece = min(64, rows)

        @pl.loop(0, rows // piece)
        def _(index):
            where = pl.ds(pl.multiple_of(index * piece, piece), piece)
            dst[where, :] = normed(src[where, :].astype(jnp.float32))

    def project_q(stage, src):
        low = stages[stage][0]

        def body(index):
            q[tile_rows(index), :] = jnp.dot(
                src[tile_rows(index), :], wall[:, low : low + width], preferred_element_type=jnp.float32
            ).astype(jnp.bfloat16)

        for_tiles(body)

    def project_kv(stage, src, slab, offset):
        low = stages[stage][0]

        def body(index):
            slab[tile_rows(index, offset), :] = jnp.dot(
                src[tile_rows(index), :],
                wall[:, low + width : low + 3 * width],
                preferred_element_type=jnp.float32,
            ).astype(jnp.bfloat16)

        for_tiles(body)

    def project_out(stage):
        low = stages[stage][0] + 3 * width

        def body(index):
            p[tile_rows(index), :] = contract_rows(
                attn[tile_rows(index), :], wall[:, low : low + width]
            ).astype(jnp.bfloat16)

        for_tiles(body)

    def attend(slab, mask, keys, moving):
        lane = lax.broadcasted_iota(jnp.int32, (BLOCK, width), 1)

        @pl.loop(0, rows // BLOCK)
        def _(index):
            where = pl.ds(pl.multiple_of(index * BLOCK, BLOCK), BLOCK)
            taken = pl.ds(pl.multiple_of(index * BLOCK, BLOCK), keys) if moving else pl.ds(0, keys)
            query = q[where, :]
            zero = jnp.zeros_like(query)
            both = jnp.concatenate(
                [jnp.where(lane < HD, query, zero), jnp.where(lane < HD, zero, query)], axis=0
            )
            scores = mask(contract_rows(both, slab[taken, 0:width]), index, where, taken)
            maxima = jnp.max(scores, axis=1, keepdims=True)
            expo = jnp.exp2((scores - maxima) * SCALE)
            totals = jnp.sum(expo, axis=1, keepdims=True)
            mixed = jnp.dot(
                expo.astype(jnp.bfloat16),
                slab[taken, width : 2 * width],
                preferred_element_type=jnp.float32,
            )
            mixed = mixed / totals
            attn[where, :] = jnp.where(lane < HD, mixed[:BLOCK], mixed[BLOCK:]).astype(jnp.bfloat16)

    def listed_mask(bias):
        def mask(scores, index, where, taken):
            return scores + bias[pl.ds(index, 1), :]

        return mask

    def window_mask(scores, index, where, taken):
        ids = query_ids[where, :]
        same = jnp.concatenate([ids, ids], axis=0) == key_ids[:, taken]
        return jnp.where(same, scores, NEGATIVE)

    def swap_sides(slab, first):
        view = slab.at[pl.ds(rows, rows), :]
        moves = [
            copy(
                view,
                slab.at[pl.ds((1 - o) * rows, rows), :],
                hs.at[first + k],
                hr.at[first + k],
                band=band(o),
            )
            for k, o in enumerate((1, -1))
        ]
        for move in moves:
            begin(move)
        return moves

    zstart(0)
    norm_rows(mesh_ref, x)
    zstep(0, 1)
    norm_rows(grid_ref, gn)
    for step in range(2, right_steps + 1):
        zstep(0, step)
    zfinish(0)
    zstart(1)
    project_kv(0, gn, eslab, rows)
    moves = swap_sides(eslab, 0)
    project_q(0, x)
    for move in moves:
        move.wait_recv()
    attend(eslab, listed_mask(enc_bias), 3 * rows, False)
    project_out(0)
    mine = share_rows(h)
    state[...] = mesh_ref[mine, :].astype(jnp.float32) + summed(0, 1)
    x[mine, :] = normed(state[...])
    gathered(0, 1)

    zstart(2)
    project_kv(1, x, wslab, REACH * rows)
    view = wslab.at[pl.ds(REACH * rows, rows), :]

    def part(place):
        return wslab.at[pl.ds(pl.multiple_of(place * rows, rows), rows), :]

    moves = [
        copy(view, part(1), hs.at[2], hr.at[2], band=band(2)),
        copy(view, part(5), hs.at[3], hr.at[3], band=band(-2)),
        copy(view, part(2 + 2 * odd), hs.at[4], hr.at[4], band=partner),
        copy(view, part(6 - 6 * odd), hs.at[5], hr.at[5], band=lax.rem(b + 6 * odd - 3 + nb, nb)),
    ]
    for move in moves:
        begin(move)
    project_q(1, x)
    passed = [
        copy(part(1), part(2 * odd), hs.at[6], hr.at[6], band=partner),
        copy(part(5), part(4 + 2 * odd), hs.at[7], hr.at[7], band=partner),
    ]
    for move, onward in zip(moves, passed):
        move.wait_recv()
        begin(onward)
    for move in (moves[2], moves[3], *passed):
        move.wait_recv()
    attend(wslab, window_mask, 2 * REACH * rows + BLOCK, True)
    project_out(1)
    state[...] = state[...] + summed(1, 2)
    x[mine, :] = normed(state[...])
    gathered(1, 2)

    zstart(3)
    low = stages[2][0]

    def feed(index):
        inner = jnp.dot(
            x[tile_rows(index), :], wall[:, low : low + ff], preferred_element_type=jnp.float32
        )
        hidden[tile_rows(index), :] = (inner * 0.5 * (1.0 + lax.erf(inner * 0.5**0.5))).astype(
            jnp.bfloat16
        )
        p[tile_rows(index), :] = contract_rows(
            hidden[tile_rows(index), :], wall[:, low + ff : low + 2 * ff]
        ).astype(jnp.bfloat16)

    for_tiles(feed)
    state[...] = state[...] + summed(2, 3)
    x[mine, :] = normed(state[...])
    gathered(2, 3)

    project_kv(3, x, dslab, rows)
    moves = swap_sides(dslab, 8)
    project_q(3, gn)
    for move in moves:
        move.wait_recv()
    attend(dslab, listed_mask(dec_bias), 3 * rows, False)
    project_out(3)
    out_ref[...] = (grid_ref[mine, :].astype(jnp.float32) + summed(3, None)).astype(jnp.bfloat16)
    for move in sent:
        move.wait_send()


def listed_bias(lists, counts, b, blocks, keys_per_block):
    my_lists = lax.dynamic_slice_in_dim(lists, b * blocks, blocks, 0) - (b - 1) * keys_per_block
    my_counts = lax.dynamic_slice_in_dim(counts, b * blocks, blocks, 0)
    live = jnp.arange(lists.shape[1], dtype=jnp.int32)[None, :] < my_counts[:, None]
    places = jnp.arange(3 * keys_per_block * BLOCK, dtype=jnp.int32) // BLOCK
    hit = (my_lists[:, :, None] == places[None, None, :]) & live[:, :, None]
    return jnp.where(jnp.any(hit, axis=1), 0.0, NEGATIVE).astype(jnp.float32)


def per_device(
    nb,
    nh,
    grid_feats,
    mesh_feats,
    enc_in,
    enc_out,
    proc_in,
    proc_out,
    ff_up,
    ff_down,
    dec_in,
    dec_out,
    enc_list,
    enc_count,
    dec_list,
    dec_count,
    window_ids,
):
    b = lax.axis_index("band")
    rows, depth = mesh_feats.shape
    assert grid_feats.shape == mesh_feats.shape and WINDOW <= REACH * rows
    width = enc_in.shape[2]
    ff = ff_up.shape[1]
    share = rows // nh
    nz = nb // 2
    w = jnp.concatenate(
        [
            *(enc_in[k] for k in range(3)),
            enc_out.T,
            *(proc_in[k] for k in range(3)),
            proc_out.T,
            ff_up,
            ff_down.T,
            *(dec_in[k] for k in range(3)),
            dec_out.T,
        ],
        axis=1,
    )
    blocks = rows // BLOCK
    enc_bias = listed_bias(enc_list, enc_count, b, blocks, blocks)
    dec_bias = listed_bias(dec_list, dec_count, b, blocks, blocks)
    padded = jnp.pad(window_ids, (REACH * rows, REACH * rows), constant_values=-1)
    key_ids = lax.dynamic_slice_in_dim(padded, b * rows, (2 * REACH + 1) * rows, 0)[None, :]
    query_ids = lax.dynamic_slice_in_dim(window_ids, b * rows, rows, 0)[:, None]
    bf16, f32 = jnp.bfloat16, jnp.float32
    dma = pltpu.SemaphoreType.DMA
    msgs = 2 * (nh - 1)
    vmem = pl.BlockSpec(memory_space=pltpu.VMEM)
    return pl.pallas_call(
        functools.partial(kernel, nb, nh),
        out_shape=jax.ShapeDtypeStruct((share, depth), bf16),
        in_specs=[vmem] * 7,
        out_specs=vmem,
        scratch_shapes=[
            pltpu.VMEM((nb * w.shape[0], w.shape[1]), bf16),
            pltpu.VMEM((rows, depth), bf16),
            pltpu.VMEM((rows, depth), bf16),
            pltpu.VMEM((rows, width), bf16),
            pltpu.VMEM((rows, width), bf16),
            pltpu.VMEM((rows, ff), bf16),
            pltpu.VMEM((rows, depth), bf16),
            pltpu.VMEM((msgs, share, depth // 2), bf16),
            pltpu.VMEM((3 * rows, 2 * width), bf16),
            pltpu.VMEM(((2 * REACH + 1) * rows, 2 * width), bf16),
            pltpu.VMEM((3 * rows, 2 * width), bf16),
            pltpu.VMEM((share, depth), f32),
            dma((4, 2, nz // 2)),
            dma((4, 2, nz // 2)),
            dma((4, nz)),
            dma((4, nz)),
            dma((4, msgs)),
            dma((4, msgs)),
            dma((3, msgs)),
            dma((3, msgs)),
            dma((10,)),
            dma((10,)),
        ],
        compiler_params=pltpu.CompilerParams(
            collective_id=0, has_side_effects=True, vmem_limit_bytes=60 * 1024 * 1024
        ),
    )(grid_feats, mesh_feats, w, enc_bias, dec_bias, key_ids, query_ids)


def solution(mesh):
    rows = P(("members", "band"), None)
    placed = (
        rows,
        rows,
        P(None, "band", "head"),
        P("head", "band"),
        P(None, "band", "head"),
        P("head", "band"),
        P("band", "head"),
        P("head", "band"),
        P(None, "band", "head"),
        P("head", "band"),
        P(),
        P(),
        P(),
        P(),
        P(),
    )
    return jax.shard_map(
        functools.partial(per_device, mesh.shape["band"], mesh.shape["head"]),
        mesh=mesh,
        in_specs=placed,
        out_specs=P(("members", "band", "head"), None),
        check_vma=False,
    )
```

```python
import functools

import jax
import jax.numpy as jnp
from jax import lax
from jax.experimental import pallas as pl
from jax.experimental.pallas import tpu as pltpu
from jax.sharding import PartitionSpec as P

HD = 64
BLOCK = 128
WINDOW = 1536
REACH = 3
GROUPS = 2
EPSILON = 1e-05
NEGATIVE = -1e30
SCALE = HD ** (-0.5) * 1.4426950408889634
MESH_ID = pl.DeviceIdType.MESH


def contract_rows(left, right):
    return lax.dot_general(left, right, (((1,), (1,)), ((), ())), preferred_element_type=jnp.float32)


def normed(values):
    centred = values - jnp.mean(values, axis=-1, keepdims=True)
    variance = jnp.mean(centred * centred, axis=-1, keepdims=True)
    return (centred * lax.rsqrt(variance + EPSILON)).astype(jnp.bfloat16)


def kernel(
    nb,
    nh,
    grid_ref,
    mesh_ref,
    w_ref,
    enc_bias,
    dec_bias,
    key_ids,
    query_ids,
    out_ref,
    wall,
    x,
    gn,
    q,
    p,
    slots,
    eslab,
    wslab,
    dslab,
    state,
    zs,
    zr,
    ps,
    pr,
    rss,
    rsr,
    ags,
    agr,
    hs,
    hr,
):
    b = lax.axis_index("band")
    h = lax.axis_index("head")
    rows, depth = grid_ref.shape
    width = q.shape[1]
    ff = (w_ref.shape[1] - 12 * width) // 2
    share = rows // nh
    half_cols = depth // 2
    wrows = w_ref.shape[0]
    nz = nb // 2
    odd = lax.rem(b, 2)
    partner = b + 1 - 2 * odd
    stages = (
        (0, 4 * width),
        (4 * width, 8 * width),
        (8 * width, 8 * width + 2 * ff),
        (8 * width + 2 * ff, 12 * width + 2 * ff),
    )

    def band(offset):
        return lax.rem(b + (offset + nb), nb)

    def head(offset):
        return lax.rem(h + (offset + nh), nh)

    def copy(src, dst, send_sem, recv_sem, **where):
        return pltpu.make_async_remote_copy(
            src_ref=src,
            dst_ref=dst,
            send_sem=send_sem,
            recv_sem=recv_sem,
            device_id={"band": where.get("band", b), "head": where.get("head", h)},
            device_id_type=MESH_ID,
        )

    barrier = pltpu.get_barrier_semaphore()
    peers = [{"band": band(o), "head": h} for o in (1, -1, 2, -2, 3, -3)]
    peers += [{"band": b, "head": head(o)} for o in (1, -1)]
    for peer in peers:
        pl.semaphore_signal(barrier, inc=1, device_id=peer, device_id_type=MESH_ID)
    pl.semaphore_wait(barrier, len(peers))

    right_steps = nz // 2
    left_steps = nz - 1 - right_steps

    def block(index, stage):
        low, high = stages[stage]
        return wall.at[pl.ds(pl.multiple_of(index * wrows, wrows), wrows), low:high]

    def own(stage):
        low, high = stages[stage]
        return w_ref.at[:, low:high]

    def zcopy(stage, way, step, first=False):
        index = band(2 * step if way else -2 * step)
        return copy(
            own(stage) if first else block(index, stage),
            block(index, stage),
            zs.at[stage, way, step],
            zr.at[stage, way, step],
            band=band(-2 if way else 2),
        )

    def pcopy(stage, k, first=False):
        index = band(2 * k)
        src = own(stage) if first else block(index, stage)
        return copy(src, block(index, stage), ps.at[stage, k], pr.at[stage, k], band=partner)

    def zstart(stage):
        zcopy(stage, 0, 0, True).start()
        if left_steps:
            zcopy(stage, 1, 0, True).start()
        pcopy(stage, 0, True).start()
        low, high = stages[stage]
        wall[pl.ds(pl.multiple_of(b * wrows, wrows), wrows), low:high] = w_ref[:, low:high]

    def zstep(stage, step):
        if isinstance(step, int):
            when = lambda condition: (lambda body: body() if condition else None)
        else:
            when = pl.when

        @when(step <= right_steps)
        def _():
            zcopy(stage, 0, step - 1).wait_recv()

            @when(step < right_steps)
            def _():
                zcopy(stage, 0, step).start()

            pcopy(stage, nz - step).start()

            @when(step <= left_steps)
            def _():
                zcopy(stage, 1, step - 1).wait_recv()

                @when(step < left_steps)
                def _():
                    zcopy(stage, 1, step).start()

                pcopy(stage, step).start()

    def zfinish(stage):
        for k in range(nz):
            pcopy(stage, k).wait_recv()
        for k in range(nz):
            pcopy(stage, k).wait_send()
        for way, steps in enumerate((right_steps, left_steps)):
            for step in range(steps):
                zcopy(stage, way, step).wait_send()

    longer = nh // 2
    shorter = nh - 1 - longer
    flows = ((1, 0, longer), (-1, 1, longer), (1, 1, shorter), (-1, 0, shorter))
    base = (0, longer, 2 * longer, 2 * longer + shorter)
    piece = share // GROUPS

    def share_rows(chunk, offset=0):
        return pl.ds(pl.multiple_of(offset + chunk * share, share), share)

    def piece_rows(chunk, group):
        return pl.ds(pl.multiple_of(chunk * share + group * piece, piece), piece)

    def half_of(half):
        return slice(half * half_cols, (half + 1) * half_cols)

    def rcopy(stage, group, flow, step):
        way, half, hops = flows[flow]
        slot = base[flow] + step
        return copy(
            p.at[stage % 2, piece_rows(head(way * (hops - step)), group), half_of(half)],
            slots.at[group, slot],
            rss.at[stage, group, slot],
            rsr.at[stage, group, slot],
            head=head(way),
        )

    def acopy(stage, group, flow, step):
        way, half, hops = flows[flow]
        slot = base[flow] + step
        view = x.at[piece_rows(head(-way * step), group), half_of(half)]
        return copy(
            view, view, ags.at[stage, group, slot], agr.at[stage, group, slot], head=head(way)
        )

    def scattered(stage, produce, ticks):
        @pl.loop(0, longer)
        def _(i):
            produce(i)
            for group in range(GROUPS):
                for flow, (way, half, hops) in enumerate(flows):
                    lag = longer - hops

                    def go(group=group, flow=flow, way=way, half=half, hops=hops, lag=lag):
                        step = i - lag

                        @pl.when(step > 0)
                        def _():
                            rcopy(stage, group, flow, step - 1).wait_recv()
                            where = piece_rows(head(way * (hops - step)), group)
                            p[stage % 2, where, half_of(half)] = (
                                p[stage % 2, where, half_of(half)].astype(jnp.float32)
                                + slots[group, base[flow] + step - 1].astype(jnp.float32)
                            ).astype(jnp.bfloat16)

                        rcopy(stage, group, flow, step).start()

                    if lag:
                        pl.when(i >= lag)(go)
                    else:
                        go()
            for z_stage, first in ticks:
                zstep(z_stage, first + i)

    def summed(stage, group):
        halves = [
            p[stage % 2, piece_rows(h, group), half_of(half)].astype(jnp.float32)
            for half in range(2)
        ]
        for flow, (way, half, hops) in enumerate(flows):
            rcopy(stage, group, flow, hops - 1).wait_recv()
            halves[half] = halves[half] + slots[group, base[flow] + hops - 1].astype(jnp.float32)
        return jnp.concatenate(halves, axis=1)

    def spread(stage, group, step):
        for flow, (way, half, hops) in enumerate(flows):
            if 1 <= step <= hops:
                acopy(stage, group, flow, step - 1).wait_recv()
            if step < hops:
                acopy(stage, group, flow, step).start()

    def settled(stage, with_gather=True):
        for group in range(GROUPS):
            for flow, (way, half, hops) in enumerate(flows):
                for step in range(hops):
                    rcopy(stage, group, flow, step).wait_send()
                    if with_gather:
                        acopy(stage, group, flow, step).wait_send()

    def arrived(step):
        if step == 0:
            return [h]
        if step <= shorter:
            return [head(-step), head(step)]
        return [head(step)]

    def rows_at(step):
        return jnp.concatenate([x[share_rows(c), :] for c in arrived(step)], axis=0)

    def finish(stage, residual, events):
        for group in range(GROUPS):
            state_rows = pl.ds(group * piece, piece)
            total = summed(stage, group) + residual(group)
            state[state_rows, :] = total
            x[piece_rows(h, group), :] = normed(total)
            spread(stage, group, 0)
        events(0)
        for step in range(1, longer + 1):
            for group in range(GROUPS):
                spread(stage, group, step)
            events(step)
        settled(stage)

    tile = min(256, rows)
    tiles = rows // tile

    def tile_rows(index, offset=0):
        return pl.ds(pl.multiple_of(offset + index * tile, tile), tile)

    def for_tiles(body):
        @pl.loop(0, tiles)
        def _(index):
            body(index)

    def norm_rows(src, dst):
        some = min(64, rows)

        @pl.loop(0, rows // some)
        def _(index):
            where = pl.ds(pl.multiple_of(index * some, some), some)
            dst[where, :] = normed(src[where, :].astype(jnp.float32))

    def project_q(stage, src):
        low = stages[stage][0]

        def body(index):
            q[tile_rows(index), :] = jnp.dot(
                src[tile_rows(index), :], wall[:, low : low + width], preferred_element_type=jnp.float32
            ).astype(jnp.bfloat16)

        for_tiles(body)

    def project_kv(stage, src, slab, offset):
        low = stages[stage][0]

        def body(index):
            slab[tile_rows(index, offset), :] = jnp.dot(
                src[tile_rows(index), :],
                wall[:, low + width : low + 3 * width],
                preferred_element_type=jnp.float32,
            ).astype(jnp.bfloat16)

        for_tiles(body)

    blocks = rows // BLOCK

    def block_at(i):
        farthest = lax.rem(h + nh // 2, nh) // (BLOCK // share)
        away = (i + 1) // 2 * (1 - 2 * lax.rem(i, 2)) * (1 - 2 * lax.rem(h, 2))
        return lax.rem(farthest + away + blocks, blocks)

    def attend(stage, index, slab, mask, keys, moving):
        lane = lax.broadcasted_iota(jnp.int32, (BLOCK, width), 1)
        where = pl.ds(pl.multiple_of(index * BLOCK, BLOCK), BLOCK)
        taken = pl.ds(pl.multiple_of(index * BLOCK, BLOCK), keys) if moving else pl.ds(0, keys)
        query = q[where, :]
        zero = jnp.zeros_like(query)
        both = jnp.concatenate(
            [jnp.where(lane < HD, query, zero), jnp.where(lane < HD, zero, query)], axis=0
        )
        scores = mask(contract_rows(both, slab[taken, 0:width]), index, where, taken)
        maxima = jnp.max(scores, axis=1, keepdims=True)
        expo = jnp.exp2((scores - maxima) * SCALE)
        totals = jnp.sum(expo, axis=1, keepdims=True)
        mixed = jnp.dot(
            expo.astype(jnp.bfloat16),
            slab[taken, width : 2 * width],
            preferred_element_type=jnp.float32,
        )
        mixed = mixed / totals
        mixed = jnp.where(lane < HD, mixed[:BLOCK], mixed[BLOCK:]).astype(jnp.bfloat16)
        low = stages[stage][0] + 3 * width
        p[stage % 2 if stage < 2 else 1, where, :] = contract_rows(
            mixed, wall[:, low : low + width]
        ).astype(jnp.bfloat16)

    def listed_mask(bias):
        def mask(scores, index, where, taken):
            return scores + bias[pl.ds(index, 1), :]

        return mask

    def window_mask(scores, index, where, taken):
        ids = query_ids[where, :]
        same = jnp.concatenate([ids, ids], axis=0) == key_ids[:, taken]
        return jnp.where(same, scores, NEGATIVE)

    def side(slab, o, first, where=None):
        k = 0 if o == 1 else 1
        start, count = (0, rows) if where is None else where
        return copy(
            slab.at[pl.ds(pl.multiple_of(rows + start, share), count), :],
            slab.at[pl.ds(pl.multiple_of((1 - o) * rows + start, share), count), :],
            hs.at[first + k],
            hr.at[first + k],
            band=band(o),
        )

    zstart(0)
    norm_rows(mesh_ref, x)
    zstep(0, 1)
    norm_rows(grid_ref, gn)
    for step in range(2, right_steps + 1):
        zstep(0, step)
    zfinish(0)
    project_kv(0, gn, eslab, rows)
    for o in (1, -1):
        side(eslab, o, 0).start()
    zstart(1)
    project_q(0, x)
    zstep(1, 1)
    for o in (1, -1):
        side(eslab, o, 0).wait_recv()
    zstep(1, 2)

    def encode(i):
        attend(0, block_at(i), eslab, listed_mask(enc_bias), 3 * rows, False)

    scattered(0, encode, ((1, 3),))

    def mesh_rows(group):
        return mesh_ref[piece_rows(h, group), :].astype(jnp.float32)

    def state_rows(group):
        return state[pl.ds(group * piece, piece), :]

    def part(place, where=None):
        start, count = (0, rows) if where is None else where
        return wslab.at[pl.ds(pl.multiple_of(place * rows + start, share), count), :]

    def window_moves(where=None):
        view = part(REACH, where)
        far = lax.rem(b + 6 * odd - 3 + nb, nb)
        return (
            copy(view, part(1, where), hs.at[2], hr.at[2], band=band(2)),
            copy(view, part(5, where), hs.at[3], hr.at[3], band=band(-2)),
            copy(view, part(6 - 6 * odd, where), hs.at[5], hr.at[5], band=far),
            copy(view, part(2 + 2 * odd, where), hs.at[4], hr.at[4], band=partner),
        )

    def proc_rows(step):
        low = stages[1][0]
        made = jnp.dot(
            rows_at(step), wall[:, low : low + 3 * width], preferred_element_type=jnp.float32
        ).astype(jnp.bfloat16)
        for k, chunk in enumerate(arrived(step)):
            mine = made[k * share : (k + 1) * share]
            q[share_rows(chunk), :] = mine[:, :width]
            wslab[share_rows(chunk, REACH * rows), :] = mine[:, width:]
            for move in window_moves((chunk * share, share)):
                move.start()

    def after_encoder(step):
        if step == 0:
            zstep(1, longer + 3)
            return
        if step == 1:
            for late in range(longer + 4, right_steps + 1):
                zstep(1, late)
            zfinish(1)
            proc_rows(0)
        proc_rows(step)

    finish(0, mesh_rows, after_encoder)

    zstart(2)
    moves = window_moves()
    passed = (
        copy(part(1), part(2 * odd), hs.at[6], hr.at[6], band=partner),
        copy(part(5), part(4 + 2 * odd), hs.at[7], hr.at[7], band=partner),
    )
    for move, onward in zip(moves, passed):
        move.wait_recv()
        onward.start()
    zstep(2, 1)
    for move in (moves[3], moves[2], *passed):
        move.wait_recv()

    def process(i):
        attend(1, block_at(i), wslab, window_mask, 2 * REACH * rows + BLOCK, True)

    scattered(1, process, ((2, 2),))

    def after_processor(step):
        if step == 0:
            zstart(3)
        else:
            zstep(3, step)
        zstep(2, longer + 2 + step)

    finish(1, state_rows, after_processor)
    for late in range(2 * longer + 3, right_steps + 1):
        zstep(2, late)
    zfinish(2)

    def feed(i):
        low = stages[2][0]
        where = pl.ds(pl.multiple_of(block_at(i) * BLOCK, BLOCK), BLOCK)
        inner = jnp.dot(x[where, :], wall[:, low : low + ff], preferred_element_type=jnp.float32)
        hidden = (inner * 0.5 * (1.0 + lax.erf(inner * 0.5**0.5))).astype(jnp.bfloat16)
        p[0, where, :] = contract_rows(hidden, wall[:, low + ff : low + 2 * ff]).astype(jnp.bfloat16)

    scattered(2, feed, ((3, longer + 1),))
    for late in range(2 * longer + 1, right_steps + 1):
        zstep(3, late)
    zfinish(3)

    def dec_rows(step):
        low = stages[3][0]
        made = jnp.dot(
            rows_at(step), wall[:, low + width : low + 3 * width], preferred_element_type=jnp.float32
        ).astype(jnp.bfloat16)
        for k, chunk in enumerate(arrived(step)):
            dslab[share_rows(chunk, rows), :] = made[k * share : (k + 1) * share]
            for o in (1, -1):
                side(dslab, o, 8, (chunk * share, share)).start()

    finish(2, state_rows, dec_rows)

    project_q(3, gn)
    for o in (1, -1):
        side(dslab, o, 8).wait_recv()

    def decode(i):
        attend(3, block_at(i), dslab, listed_mask(dec_bias), 3 * rows, False)

    scattered(3, decode, ())
    for group in range(GROUPS):
        residual = grid_ref[piece_rows(h, group), :].astype(jnp.float32)
        out_ref[pl.ds(group * piece, piece), :] = (residual + summed(3, group)).astype(jnp.bfloat16)
    settled(3, False)
    for o in (1, -1):
        side(eslab, o, 0).wait_send()
        side(dslab, o, 8).wait_send()
    for move in (*moves, *passed):
        move.wait_send()


def listed_bias(lists, counts, b, blocks, keys_per_block):
    my_lists = lax.dynamic_slice_in_dim(lists, b * blocks, blocks, 0) - (b - 1) * keys_per_block
    my_counts = lax.dynamic_slice_in_dim(counts, b * blocks, blocks, 0)
    live = jnp.arange(lists.shape[1], dtype=jnp.int32)[None, :] < my_counts[:, None]
    places = jnp.arange(3 * keys_per_block * BLOCK, dtype=jnp.int32) // BLOCK
    hit = (my_lists[:, :, None] == places[None, None, :]) & live[:, :, None]
    return jnp.where(jnp.any(hit, axis=1), 0.0, NEGATIVE).astype(jnp.float32)


def per_device(
    nb,
    nh,
    grid_feats,
    mesh_feats,
    enc_in,
    enc_out,
    proc_in,
    proc_out,
    ff_up,
    ff_down,
    dec_in,
    dec_out,
    enc_list,
    enc_count,
    dec_list,
    dec_count,
    window_ids,
):
    b = lax.axis_index("band")
    rows, depth = mesh_feats.shape
    assert grid_feats.shape == mesh_feats.shape and WINDOW <= REACH * rows
    assert nh == rows // BLOCK * 2
    width = enc_in.shape[2]
    ff = ff_up.shape[1]
    share = rows // nh
    nz = nb // 2
    w = jnp.concatenate(
        [
            *(enc_in[k] for k in range(3)),
            enc_out.T,
            *(proc_in[k] for k in range(3)),
            proc_out.T,
            ff_up,
            ff_down.T,
            *(dec_in[k] for k in range(3)),
            dec_out.T,
        ],
        axis=1,
    )
    blocks = rows // BLOCK
    enc_bias = listed_bias(enc_list, enc_count, b, blocks, blocks)
    dec_bias = listed_bias(dec_list, dec_count, b, blocks, blocks)
    padded = jnp.pad(window_ids, (REACH * rows, REACH * rows), constant_values=-1)
    key_ids = lax.dynamic_slice_in_dim(padded, b * rows, (2 * REACH + 1) * rows, 0)[None, :]
    query_ids = lax.dynamic_slice_in_dim(window_ids, b * rows, rows, 0)[:, None]
    bf16, f32 = jnp.bfloat16, jnp.float32
    dma = pltpu.SemaphoreType.DMA
    msgs = 2 * (nh - 1)
    vmem = pl.BlockSpec(memory_space=pltpu.VMEM)
    return pl.pallas_call(
        functools.partial(kernel, nb, nh),
        out_shape=jax.ShapeDtypeStruct((share, depth), bf16),
        in_specs=[vmem] * 7,
        out_specs=vmem,
        scratch_shapes=[
            pltpu.VMEM((nb * w.shape[0], w.shape[1]), bf16),
            pltpu.VMEM((rows, depth), bf16),
            pltpu.VMEM((rows, depth), bf16),
            pltpu.VMEM((rows, width), bf16),
            pltpu.VMEM((2, rows, depth), bf16),
            pltpu.VMEM((GROUPS, msgs, share // GROUPS, depth // 2), bf16),
            pltpu.VMEM((3 * rows, 2 * width), bf16),
            pltpu.VMEM(((2 * REACH + 1) * rows, 2 * width), bf16),
            pltpu.VMEM((3 * rows, 2 * width), bf16),
            pltpu.VMEM((share, depth), f32),
            dma((4, 2, nz // 2)),
            dma((4, 2, nz // 2)),
            dma((4, nz)),
            dma((4, nz)),
            dma((4, GROUPS, msgs)),
            dma((4, GROUPS, msgs)),
            dma((3, GROUPS, msgs)),
            dma((3, GROUPS, msgs)),
            dma((10,)),
            dma((10,)),
        ],
        compiler_params=pltpu.CompilerParams(
            collective_id=0, has_side_effects=True, vmem_limit_bytes=60 * 1024 * 1024
        ),
    )(grid_feats, mesh_feats, w, enc_bias, dec_bias, key_ids, query_ids)


def solution(mesh):
    rows = P(("members", "band"), None)
    placed = (
        rows,
        rows,
        P(None, "band", "head"),
        P("head", "band"),
        P(None, "band", "head"),
        P("head", "band"),
        P("band", "head"),
        P("head", "band"),
        P(None, "band", "head"),
        P("head", "band"),
        P(),
        P(),
        P(),
        P(),
        P(),
    )
    return jax.shard_map(
        functools.partial(per_device, mesh.shape["band"], mesh.shape["head"]),
        mesh=mesh,
        in_specs=placed,
        out_specs=P(("members", "band", "head"), None),
        check_vma=False,
    )
```

```python
import functools

import jax
import jax.numpy as jnp
from jax import lax
from jax.experimental import pallas as pl
from jax.experimental.pallas import tpu as pltpu
from jax.sharding import PartitionSpec as P

HD = 64
BLOCK = 128
WINDOW = 1536
REACH = 3
GROUPS = 2
EPSILON = 1e-05
NEGATIVE = -1e30
SCALE = HD ** (-0.5) * 1.4426950408889634
MESH_ID = pl.DeviceIdType.MESH


def contract_rows(left, right):
    return lax.dot_general(left, right, (((1,), (1,)), ((), ())), preferred_element_type=jnp.float32)


def normed(values):
    centred = values - jnp.mean(values, axis=-1, keepdims=True)
    variance = jnp.mean(centred * centred, axis=-1, keepdims=True)
    return (centred * lax.rsqrt(variance + EPSILON)).astype(jnp.bfloat16)


def kernel(
    nb,
    nh,
    grid_ref,
    mesh_ref,
    enc_in,
    enc_out,
    proc_in,
    proc_out,
    ff_up,
    ff_down,
    dec_in,
    dec_out,
    enc_list,
    enc_count,
    dec_list,
    dec_count,
    ids,
    out_ref,
    wall,
    x,
    gn,
    q,
    p,
    slots,
    eslab,
    wslab,
    dslab,
    state,
    enc_bias,
    dec_bias,
    key_ids,
    query_ids,
    zs,
    zr,
    pr,
    rss,
    rsr,
    ags,
    agr,
    hs,
    hr,
):
    b = lax.axis_index("band")
    h = lax.axis_index("head")
    rows, depth = grid_ref.shape
    width = q.shape[1]
    ff = ff_up.shape[1]
    share = rows // nh
    half_cols = depth // 2
    wrows = ff_up.shape[0]
    nz = nb // 2
    odd = lax.rem(b, 2)
    partner = b + 1 - 2 * odd
    stages = (
        (0, 4 * width),
        (4 * width, 8 * width),
        (8 * width, 8 * width + 2 * ff),
        (8 * width + 2 * ff, 12 * width + 2 * ff),
    )

    def band(offset):
        return lax.rem(b + (offset + nb), nb)

    def head(offset):
        return lax.rem(h + (offset + nh), nh)

    def copy(src, dst, send_sem, recv_sem, **where):
        return pltpu.make_async_remote_copy(
            src_ref=src,
            dst_ref=dst,
            send_sem=send_sem,
            recv_sem=recv_sem,
            device_id={"band": where.get("band", b), "head": where.get("head", h)},
            device_id_type=MESH_ID,
        )

    place = 0
    own_rows = pl.ds(pl.multiple_of(b * wrows, wrows), wrows)
    for three, out in ((enc_in, enc_out), (proc_in, proc_out), (ff_up, ff_down), (dec_in, dec_out)):
        pieces = [three[k] for k in range(3)] if len(three.shape) == 3 else [three[...]]
        for one in (*pieces, out[...]):
            wall[own_rows, place : place + one.shape[1]] = one
            place += one.shape[1]

    barrier = pltpu.get_barrier_semaphore()
    peers = [{"band": band(o), "head": h} for o in (1, -1, 2, -2, 3, -3, 4, -4)]
    peers += [{"band": b, "head": head(o)} for o in (1, -1)]
    for peer in peers:
        pl.semaphore_signal(barrier, inc=1, device_id=peer, device_id_type=MESH_ID)
    pl.semaphore_wait(barrier, len(peers))

    reaches = (nz // 2, nz - 1 - nz // 2)
    z_steps = (reaches[0] + 1) // 2

    def wall_rows(start, count, stage):
        low, high = stages[stage]
        return wall.at[pl.ds(pl.multiple_of(start * wrows, wrows), count * wrows), low:high]

    def zcopy(stage, way, near, step):
        side_of = -1 if way else 1
        view = wall_rows(band(-4 * side_of * step), 1, stage)
        return copy(
            view,
            view,
            zs.at[stage],
            zr.at[stage, way, near, step],
            band=band(side_of * (2 if near else 4)),
        )

    def hand_over(stage, way, distance):
        view = wall_rows(band(2 * distance if way else -2 * distance), 1, stage)
        copy(view, view, zs.at[stage], pr.at[stage], band=partner).start()

    def zstart(stage):
        for way, reach in enumerate(reaches):
            if reach >= 2:
                zcopy(stage, way, 0, 0).start()
            if reach >= 1:
                zcopy(stage, way, 1, 0).start()
        hand_over(stage, 0, 0)

    def zstep(stage, step):
        if isinstance(step, int):
            when = lambda condition: (lambda body: body() if condition else None)
        else:
            when = pl.when
        for way, reach in enumerate(reaches):

            @when(2 * step <= reach)
            def _(way=way, reach=reach):
                zcopy(stage, way, 0, step - 1).wait_recv()

                @when(2 * step + 2 <= reach)
                def _():
                    zcopy(stage, way, 0, step).start()

                @when(2 * step + 1 <= reach)
                def _():
                    zcopy(stage, way, 1, step).start()

        for way, reach in enumerate(reaches):

            @when(2 * step <= reach)
            def _(way=way):
                hand_over(stage, way, 2 * step)

            @when(2 * step - 1 <= reach)
            def _(way=way):
                zcopy(stage, way, 1, step - 1).wait_recv()
                hand_over(stage, way, 2 * step - 1)

    def zfinish(stage):
        whole = wall_rows(0, nz, stage)
        copy(whole, whole, zs.at[stage], pr.at[stage]).wait_recv()

    def zsettle(stage):
        whole = wall_rows(0, 2 * nz - 1, stage)
        copy(whole, whole, zs.at[stage], pr.at[stage]).wait_send()

    longer = nh // 2
    shorter = nh - 1 - longer
    flows = ((1, 0, longer), (-1, 1, longer), (1, 1, shorter), (-1, 0, shorter))
    base = (0, longer, 2 * longer, 2 * longer + shorter)
    piece = share // GROUPS

    def share_rows(chunk, offset=0):
        return pl.ds(pl.multiple_of(offset + chunk * share, share), share)

    def piece_rows(chunk, group):
        return pl.ds(pl.multiple_of(chunk * share + group * piece, piece), piece)

    def half_of(half):
        return slice(half * half_cols, (half + 1) * half_cols)

    def rcopy(stage, group, flow, step):
        way, half, hops = flows[flow]
        slot = base[flow] + step
        return copy(
            p.at[stage % 2, piece_rows(head(way * (hops - step)), group), half_of(half)],
            slots.at[group, slot],
            rss.at[0],
            rsr.at[group, slot],
            head=head(way),
        )

    def acopy(stage, group, flow, step):
        way, half, hops = flows[flow]
        slot = base[flow] + step
        view = x.at[piece_rows(head(-way * step), group), half_of(half)]
        return copy(view, view, ags.at[0], agr.at[group, slot], head=head(way))

    def scattered(stage, produce, ticks):
        @pl.loop(0, longer)
        def _(i):
            produce(i)
            for group in range(GROUPS):
                for flow, (way, half, hops) in enumerate(flows):
                    lag = longer - hops

                    def go(group=group, flow=flow, way=way, half=half, hops=hops, lag=lag):
                        step = i - lag

                        @pl.when(step > 0)
                        def _():
                            rcopy(stage, group, flow, step - 1).wait_recv()
                            where = piece_rows(head(way * (hops - step)), group)
                            p[stage % 2, where, half_of(half)] = (
                                p[stage % 2, where, half_of(half)].astype(jnp.float32)
                                + slots[group, base[flow] + step - 1].astype(jnp.float32)
                            ).astype(jnp.bfloat16)

                        rcopy(stage, group, flow, step).start()

                    if lag:
                        pl.when(i >= lag)(go)
                    else:
                        go()
            for z_stage, first in ticks:

                @pl.when(lax.rem(i, 2) == 1)
                def _(z_stage=z_stage, first=first):
                    zstep(z_stage, first + i // 2)

    def summed(stage, group):
        halves = [
            p[stage % 2, piece_rows(h, group), half_of(half)].astype(jnp.float32)
            for half in range(2)
        ]
        for flow, (way, half, hops) in enumerate(flows):
            rcopy(stage, group, flow, hops - 1).wait_recv()
            halves[half] = halves[half] + slots[group, base[flow] + hops - 1].astype(jnp.float32)
        return jnp.concatenate(halves, axis=1)

    def spread(stage, group, step):
        for flow, (way, half, hops) in enumerate(flows):
            if 1 <= step <= hops:
                acopy(stage, group, flow, step - 1).wait_recv()
            if step < hops:
                acopy(stage, group, flow, step).start()

    def settled(with_gather=True):
        copy(slots, slots, rss.at[0], rsr.at[0, 0]).wait_send()
        if with_gather:
            copy(slots, slots, ags.at[0], agr.at[0, 0]).wait_send()

    def arrived(step):
        if step == 0:
            return [h]
        if step <= shorter:
            return [head(-step), head(step)]
        return [head(step)]

    def rows_at(step):
        return jnp.concatenate([x[share_rows(c), :] for c in arrived(step)], axis=0)

    def finish(stage, residual, events):
        for group in range(GROUPS):
            state_rows = pl.ds(group * piece, piece)
            total = summed(stage, group) + residual(group)
            state[state_rows, :] = total
            x[piece_rows(h, group), :] = normed(total)
            spread(stage, group, 0)
        events(0)
        for step in range(1, longer + 1):
            for group in range(GROUPS):
                spread(stage, group, step)
            events(step)
        settled()

    tile = min(256, rows)
    tiles = rows // tile

    def tile_rows(index, offset=0):
        return pl.ds(pl.multiple_of(offset + index * tile, tile), tile)

    def for_tiles(body):
        @pl.loop(0, tiles)
        def _(index):
            body(index)

    def norm_rows(src, dst):
        some = min(64, rows)

        @pl.loop(0, rows // some)
        def _(index):
            where = pl.ds(pl.multiple_of(index * some, some), some)
            dst[where, :] = normed(src[where, :].astype(jnp.float32))

    def project_q(stage, src):
        low = stages[stage][0]

        def body(index):
            q[tile_rows(index), :] = jnp.dot(
                src[tile_rows(index), :], wall[:, low : low + width], preferred_element_type=jnp.float32
            ).astype(jnp.bfloat16)

        for_tiles(body)

    def project_kv(stage, src, slab, offset):
        low = stages[stage][0]

        def body(index):
            slab[tile_rows(index, offset), :] = jnp.dot(
                src[tile_rows(index), :],
                wall[:, low + width : low + 3 * width],
                preferred_element_type=jnp.float32,
            ).astype(jnp.bfloat16)

        for_tiles(body)

    blocks = rows // BLOCK

    def block_at(i):
        farthest = lax.rem(h + nh // 2, nh) // (BLOCK // share)
        away = (i + 1) // 2 * (1 - 2 * lax.rem(i, 2)) * (1 - 2 * lax.rem(h, 2))
        return lax.rem(farthest + away + blocks, blocks)

    def attend(stage, index, slab, mask, keys, moving):
        lane = lax.broadcasted_iota(jnp.int32, (BLOCK, width), 1)
        where = pl.ds(pl.multiple_of(index * BLOCK, BLOCK), BLOCK)
        taken = pl.ds(pl.multiple_of(index * BLOCK, BLOCK), keys) if moving else pl.ds(0, keys)
        query = q[where, :]
        zero = jnp.zeros_like(query)
        both = jnp.concatenate(
            [jnp.where(lane < HD, query, zero), jnp.where(lane < HD, zero, query)], axis=0
        )
        scores = mask(contract_rows(both, slab[taken, 0:width]), index, where, taken)
        maxima = jnp.max(scores, axis=1, keepdims=True)
        expo = jnp.exp2((scores - maxima) * SCALE)
        totals = jnp.sum(expo, axis=1, keepdims=True)
        mixed = jnp.dot(
            expo.astype(jnp.bfloat16),
            slab[taken, width : 2 * width],
            preferred_element_type=jnp.float32,
        )
        mixed = mixed / totals
        mixed = jnp.where(lane < HD, mixed[:BLOCK], mixed[BLOCK:]).astype(jnp.bfloat16)
        low = stages[stage][0] + 3 * width
        p[stage % 2 if stage < 2 else 1, where, :] = contract_rows(
            mixed, wall[:, low : low + width]
        ).astype(jnp.bfloat16)

    def listed_mask(bias):
        def mask(scores, index, where, taken):
            return scores + bias[pl.ds(index, 1), :]

        return mask

    def window_mask(scores, index, where, taken):
        ids = query_ids[where, :]
        same = jnp.concatenate([ids, ids], axis=0) == key_ids[:, taken]
        return jnp.where(same, scores, NEGATIVE)

    def side(slab, o, first, where=None):
        k = 0 if o == 1 else 1
        start, count = (0, rows) if where is None else where
        return copy(
            slab.at[pl.ds(pl.multiple_of(rows + start, share), count), :],
            slab.at[pl.ds(pl.multiple_of((1 - o) * rows + start, share), count), :],
            hs.at[first + k],
            hr.at[first + k],
            band=band(o),
        )

    def fill_bias(lists, counts, bias):
        lane = lax.broadcasted_iota(jnp.int32, lists.shape, 1)
        slot = lax.broadcasted_iota(jnp.int32, (lists.shape[0], 1), 0).astype(jnp.float32)
        places = lax.broadcasted_iota(jnp.int32, (lists.shape[0], 3 * rows), 1)
        places = lax.shift_right_logical(places, BLOCK.bit_length() - 1).astype(jnp.float32)
        listed = lists[...].astype(jnp.float32)
        counted = counts[...].astype(jnp.float32)
        first = ((b - 1) * blocks).astype(jnp.float32)
        for index in range(blocks):
            mine = lane == b * blocks + index
            picked = jnp.sum(jnp.where(mine, listed, 0.0), axis=1, keepdims=True)
            count = jnp.sum(jnp.where(mine[:1], counted, 0.0), axis=1, keepdims=True)
            local = jnp.where(slot < count, picked - first, -1.0)
            hits = jnp.where(local == places, 0.0, NEGATIVE)
            bias[index : index + 1, :] = jnp.max(hits, axis=0, keepdims=True)

    def fill_ids():
        total = ids.shape[0]
        for k in range((2 * REACH + 1) * blocks):
            row = (b - REACH) * blocks + k
            inside = ((row >= 0) & (row < total)).astype(jnp.int32)
            found = ids[pl.ds(lax.rem(row + total, total), 1), :]
            key_ids[:, k * BLOCK : (k + 1) * BLOCK] = (found * inside + (inside - 1)).astype(
                jnp.float32
            )
        diagonal = lax.broadcasted_iota(jnp.int32, (BLOCK, BLOCK), 0) == lax.broadcasted_iota(
            jnp.int32, (BLOCK, BLOCK), 1
        )
        for k in range(blocks):
            row = key_ids[:, (REACH * blocks + k) * BLOCK : (REACH * blocks + k + 1) * BLOCK]
            query_ids[k * BLOCK : (k + 1) * BLOCK, :] = jnp.sum(
                jnp.where(diagonal, row, 0.0), axis=1, keepdims=True
            )

    zstart(0)
    zstart(1)
    norm_rows(mesh_ref, x)
    fill_bias(enc_list, enc_count, enc_bias)
    fill_bias(dec_list, dec_count, dec_bias)
    for step in range(1, z_steps + 1):
        zstep(0, step)
        if step == 1:
            norm_rows(grid_ref, gn)
            fill_ids()
        if step < z_steps:
            zstep(1, step)
    zfinish(0)
    project_kv(0, gn, eslab, rows)
    for o in (1, -1):
        side(eslab, o, 0).start()
    project_q(0, x)
    for o in (1, -1):
        side(eslab, o, 0).wait_recv()

    def encode(i):
        attend(0, block_at(i), eslab, listed_mask(enc_bias), 3 * rows, False)

    scattered(0, encode, ())
    zstep(1, z_steps)
    zfinish(1)

    def mesh_rows(group):
        return mesh_ref[piece_rows(h, group), :].astype(jnp.float32)

    def state_rows(group):
        return state[pl.ds(group * piece, piece), :]

    def part(place, where=None):
        start, count = (0, rows) if where is None else where
        return wslab.at[pl.ds(pl.multiple_of(place * rows + start, share), count), :]

    def window_moves(where=None):
        view = part(REACH, where)
        far = lax.rem(b + 6 * odd - 3 + nb, nb)
        return (
            copy(view, part(1, where), hs.at[2], hr.at[2], band=band(2)),
            copy(view, part(5, where), hs.at[3], hr.at[3], band=band(-2)),
            copy(view, part(6 - 6 * odd, where), hs.at[5], hr.at[5], band=far),
            copy(view, part(2 + 2 * odd, where), hs.at[4], hr.at[4], band=partner),
        )

    def proc_rows(step):
        low = stages[1][0]
        made = jnp.dot(
            rows_at(step), wall[:, low : low + 3 * width], preferred_element_type=jnp.float32
        ).astype(jnp.bfloat16)
        for k, chunk in enumerate(arrived(step)):
            mine = made[k * share : (k + 1) * share]
            q[share_rows(chunk), :] = mine[:, :width]
            wslab[share_rows(chunk, REACH * rows), :] = mine[:, width:]
            for move in window_moves((chunk * share, share)):
                move.start()

    finish(0, mesh_rows, proc_rows)

    zstart(2)
    moves = window_moves()
    passed = (
        copy(part(1), part(2 * odd), hs.at[6], hr.at[6], band=partner),
        copy(part(5), part(4 + 2 * odd), hs.at[7], hr.at[7], band=partner),
    )
    for move, onward in zip(moves, passed):
        move.wait_recv()
        onward.start()
    for move in (moves[3], moves[2], *passed):
        move.wait_recv()

    def process(i):
        attend(1, block_at(i), wslab, window_mask, 2 * REACH * rows + BLOCK, True)

    scattered(1, process, ((2, 1),))

    def after_processor(step):
        if step == 0:
            zstart(3)
        elif step % 2:
            zstep(2, longer // 2 + (step + 1) // 2)
        else:
            zstep(3, step // 2)

    finish(1, state_rows, after_processor)
    zfinish(2)

    def feed(i):
        low = stages[2][0]
        where = pl.ds(pl.multiple_of(block_at(i) * BLOCK, BLOCK), BLOCK)
        inner = jnp.dot(x[where, :], wall[:, low : low + ff], preferred_element_type=jnp.float32)
        hidden = (inner * 0.5 * (1.0 + lax.erf(inner * 0.5**0.5))).astype(jnp.bfloat16)
        p[0, where, :] = contract_rows(hidden, wall[:, low + ff : low + 2 * ff]).astype(jnp.bfloat16)

    scattered(2, feed, ((3, longer // 2 + 1),))
    zfinish(3)

    def dec_rows(step):
        low = stages[3][0]
        made = jnp.dot(
            rows_at(step), wall[:, low + width : low + 3 * width], preferred_element_type=jnp.float32
        ).astype(jnp.bfloat16)
        for k, chunk in enumerate(arrived(step)):
            dslab[share_rows(chunk, rows), :] = made[k * share : (k + 1) * share]
            for o in (1, -1):
                side(dslab, o, 8, (chunk * share, share)).start()

    finish(2, state_rows, dec_rows)

    project_q(3, gn)
    for o in (1, -1):
        side(dslab, o, 8).wait_recv()

    def decode(i):
        attend(3, block_at(i), dslab, listed_mask(dec_bias), 3 * rows, False)

    scattered(3, decode, ())
    for group in range(GROUPS):
        residual = grid_ref[piece_rows(h, group), :].astype(jnp.float32)
        out_ref[pl.ds(group * piece, piece), :] = (residual + summed(3, group)).astype(jnp.bfloat16)
    settled(False)
    for o in (1, -1):
        side(eslab, o, 0).wait_send()
        side(dslab, o, 8).wait_send()
    for move in (*moves, *passed):
        move.wait_send()
    for stage in range(4):
        zsettle(stage)


def per_device(
    nb,
    nh,
    grid_feats,
    mesh_feats,
    enc_in,
    enc_out,
    proc_in,
    proc_out,
    ff_up,
    ff_down,
    dec_in,
    dec_out,
    enc_list,
    enc_count,
    dec_list,
    dec_count,
    window_ids,
):
    rows, depth = mesh_feats.shape
    assert grid_feats.shape == mesh_feats.shape and WINDOW <= REACH * rows
    assert nh == rows // BLOCK * 2
    width = enc_in.shape[2]
    wrows, ff = ff_up.shape
    share = rows // nh
    nz = nb // 2
    blocks = rows // BLOCK
    given = (
        grid_feats,
        mesh_feats,
        enc_in,
        enc_out.T,
        proc_in,
        proc_out.T,
        ff_up,
        ff_down.T,
        dec_in,
        dec_out.T,
        enc_list.T,
        enc_count[None, :],
        dec_list.T,
        dec_count[None, :],
        window_ids.reshape(-1, BLOCK),
    )
    bf16, f32 = jnp.bfloat16, jnp.float32
    dma = pltpu.SemaphoreType.DMA
    msgs = 2 * (nh - 1)
    vmem = pl.BlockSpec(memory_space=pltpu.VMEM)
    return pl.pallas_call(
        functools.partial(kernel, nb, nh),
        out_shape=jax.ShapeDtypeStruct((share, depth), bf16),
        in_specs=[vmem] * len(given),
        out_specs=vmem,
        scratch_shapes=[
            pltpu.VMEM((nb * wrows, 12 * width + 2 * ff), bf16),
            pltpu.VMEM((rows, depth), bf16),
            pltpu.VMEM((rows, depth), bf16),
            pltpu.VMEM((rows, width), bf16),
            pltpu.VMEM((2, rows, depth), bf16),
            pltpu.VMEM((GROUPS, msgs, share // GROUPS, depth // 2), bf16),
            pltpu.VMEM((3 * rows, 2 * width), bf16),
            pltpu.VMEM(((2 * REACH + 1) * rows, 2 * width), bf16),
            pltpu.VMEM((3 * rows, 2 * width), bf16),
            pltpu.VMEM((share, depth), f32),
            pltpu.VMEM((blocks, 3 * rows), f32),
            pltpu.VMEM((blocks, 3 * rows), f32),
            pltpu.VMEM((1, (2 * REACH + 1) * rows), f32),
            pltpu.VMEM((rows, 1), f32),
            dma((4,)),
            dma((4, 2, 2, max(1, nz // 4))),
            dma((4,)),
            dma((1,)),
            dma((GROUPS, msgs)),
            dma((1,)),
            dma((GROUPS, msgs)),
            dma((10,)),
            dma((10,)),
        ],
        compiler_params=pltpu.CompilerParams(
            collective_id=0, has_side_effects=True, vmem_limit_bytes=60 * 1024 * 1024
        ),
    )(*given)


def solution(mesh):
    rows = P(("members", "band"), None)
    placed = (
        rows,
        rows,
        P(None, "band", "head"),
        P("head", "band"),
        P(None, "band", "head"),
        P("head", "band"),
        P("band", "head"),
        P("head", "band"),
        P(None, "band", "head"),
        P("head", "band"),
        P(),
        P(),
        P(),
        P(),
        P(),
    )
    return jax.shard_map(
        functools.partial(per_device, mesh.shape["band"], mesh.shape["head"]),
        mesh=mesh,
        in_specs=placed,
        out_specs=P(("members", "band", "head"), None),
        check_vma=False,
    )
```

```python
import functools

import jax
import jax.numpy as jnp
from jax import lax
from jax.experimental import pallas as pl
from jax.experimental.pallas import tpu as pltpu
from jax.sharding import PartitionSpec as P

HD = 64
BLOCK = 128
WINDOW = 1536
REACH = 3
GROUPS = 4
EPSILON = 1e-05
NEGATIVE = -1e30
SCALE = HD ** (-0.5) * 1.4426950408889634
MESH_ID = pl.DeviceIdType.MESH


def contract_rows(left, right):
    return lax.dot_general(left, right, (((1,), (1,)), ((), ())), preferred_element_type=jnp.float32)


def normed(values):
    centred = values - jnp.mean(values, axis=-1, keepdims=True)
    variance = jnp.mean(centred * centred, axis=-1, keepdims=True)
    return (centred * lax.rsqrt(variance + EPSILON)).astype(jnp.bfloat16)


def kernel(
    nb,
    nh,
    grid_ref,
    mesh_ref,
    enc_in,
    enc_out,
    proc_in,
    proc_out,
    ff_up,
    ff_down,
    dec_in,
    dec_out,
    enc_list,
    enc_count,
    dec_list,
    dec_count,
    ids,
    out_ref,
    wall,
    x,
    gn,
    q,
    p,
    slots,
    eslab,
    wslab,
    dslab,
    state,
    enc_bias,
    dec_bias,
    key_ids,
    query_ids,
    zs,
    zr,
    pr,
    rss,
    rsr,
    ags,
    agr,
    hs,
    hr,
):
    b = lax.axis_index("band")
    h = lax.axis_index("head")
    rows, depth = grid_ref.shape
    width = q.shape[1]
    ff = ff_up.shape[1]
    share = rows // nh
    half_cols = depth // 2
    wrows = ff_up.shape[0]
    nz = nb // 2
    odd = lax.rem(b, 2)
    partner = b + 1 - 2 * odd
    stages = (
        (0, 4 * width),
        (4 * width, 8 * width),
        (8 * width, 8 * width + 2 * ff),
        (8 * width + 2 * ff, 12 * width + 2 * ff),
    )

    def band(offset):
        return lax.rem(b + (offset + nb), nb)

    def head(offset):
        return lax.rem(h + (offset + nh), nh)

    def copy(src, dst, send_sem, recv_sem, **where):
        return pltpu.make_async_remote_copy(
            src_ref=src,
            dst_ref=dst,
            send_sem=send_sem,
            recv_sem=recv_sem,
            device_id={"band": where.get("band", b), "head": where.get("head", h)},
            device_id_type=MESH_ID,
        )

    place = 0
    own_rows = pl.ds(pl.multiple_of(b * wrows, wrows), wrows)
    for three, out in ((enc_in, enc_out), (proc_in, proc_out), (ff_up, ff_down), (dec_in, dec_out)):
        pieces = [three[k] for k in range(3)] if len(three.shape) == 3 else [three[...]]
        for one in (*pieces, out[...]):
            wall[own_rows, place : place + one.shape[1]] = one
            place += one.shape[1]

    barrier = pltpu.get_barrier_semaphore()
    peers = [{"band": band(o), "head": h} for o in (1, -1, 2, -2, 3, -3, 4, -4)]
    peers += [{"band": b, "head": head(o)} for o in (1, -1)]
    for peer in peers:
        pl.semaphore_signal(barrier, inc=1, device_id=peer, device_id_type=MESH_ID)
    pl.semaphore_wait(barrier, len(peers))

    reaches = (nz // 2, nz - 1 - nz // 2)
    z_steps = (reaches[0] + 1) // 2

    def wall_rows(start, count, stage):
        low, high = stages[stage]
        return wall.at[pl.ds(pl.multiple_of(start * wrows, wrows), count * wrows), low:high]

    def zcopy(stage, way, near, step):
        side_of = -1 if way else 1
        view = wall_rows(band(-4 * side_of * step), 1, stage)
        return copy(
            view,
            view,
            zs.at[stage],
            zr.at[stage, way, near, step],
            band=band(side_of * (2 if near else 4)),
        )

    def hand_over(stage, way, distance):
        view = wall_rows(band(2 * distance if way else -2 * distance), 1, stage)
        copy(view, view, zs.at[stage], pr.at[stage], band=partner).start()

    def zstart(stage):
        for way, reach in enumerate(reaches):
            if reach >= 2:
                zcopy(stage, way, 0, 0).start()
            if reach >= 1:
                zcopy(stage, way, 1, 0).start()
        hand_over(stage, 0, 0)

    def zstep(stage, step):
        if isinstance(step, int):
            when = lambda condition: (lambda body: body() if condition else None)
        else:
            when = pl.when
        for way, reach in enumerate(reaches):

            @when(2 * step <= reach)
            def _(way=way, reach=reach):
                zcopy(stage, way, 0, step - 1).wait_recv()

                @when(2 * step + 2 <= reach)
                def _():
                    zcopy(stage, way, 0, step).start()

                @when(2 * step + 1 <= reach)
                def _():
                    zcopy(stage, way, 1, step).start()

        for way, reach in enumerate(reaches):

            @when(2 * step <= reach)
            def _(way=way):
                hand_over(stage, way, 2 * step)

            @when(2 * step - 1 <= reach)
            def _(way=way):
                zcopy(stage, way, 1, step - 1).wait_recv()
                hand_over(stage, way, 2 * step - 1)

    def zfinish(stage):
        whole = wall_rows(0, nz, stage)
        copy(whole, whole, zs.at[stage], pr.at[stage]).wait_recv()

    def zsettle(stage):
        whole = wall_rows(0, 2 * nz - 1, stage)
        copy(whole, whole, zs.at[stage], pr.at[stage]).wait_send()

    longer = nh // 2
    shorter = nh - 1 - longer
    flows = ((1, 0, longer), (-1, 1, longer), (1, 1, shorter), (-1, 0, shorter))
    base = (0, longer, 2 * longer, 2 * longer + shorter)
    piece = share // GROUPS

    def share_rows(chunk, offset=0):
        return pl.ds(pl.multiple_of(offset + chunk * share, share), share)

    def piece_rows(chunk, group):
        return pl.ds(pl.multiple_of(chunk * share + group * piece, piece), piece)

    def half_of(half):
        return slice(half * half_cols, (half + 1) * half_cols)

    def rcopy(stage, group, flow, step):
        way, half, hops = flows[flow]
        slot = base[flow] + step
        return copy(
            p.at[stage % 2, piece_rows(head(way * (hops - step)), group), half_of(half)],
            slots.at[group, slot],
            rss.at[0],
            rsr.at[group, slot],
            head=head(way),
        )

    def acopy(stage, group, flow, step):
        way, half, hops = flows[flow]
        slot = base[flow] + step
        view = x.at[piece_rows(head(-way * step), group), half_of(half)]
        return copy(view, view, ags.at[0], agr.at[group, slot], head=head(way))

    def scattered(stage, produce, ticks):
        @pl.loop(0, longer)
        def _(i):
            produce(i)
            for group in range(GROUPS):
                for flow, (way, half, hops) in enumerate(flows):
                    lag = longer - hops

                    def go(group=group, flow=flow, way=way, half=half, hops=hops, lag=lag):
                        step = i - lag

                        @pl.when(step > 0)
                        def _():
                            rcopy(stage, group, flow, step - 1).wait_recv()
                            where = piece_rows(head(way * (hops - step)), group)
                            p[stage % 2, where, half_of(half)] = (
                                p[stage % 2, where, half_of(half)].astype(jnp.float32)
                                + slots[group, base[flow] + step - 1].astype(jnp.float32)
                            ).astype(jnp.bfloat16)

                        rcopy(stage, group, flow, step).start()

                    if lag:
                        pl.when(i >= lag)(go)
                    else:
                        go()
            for z_stage, first in ticks:

                @pl.when(lax.rem(i, 2) == 1)
                def _(z_stage=z_stage, first=first):
                    zstep(z_stage, first + i // 2)

    def summed(stage, group):
        halves = [
            p[stage % 2, piece_rows(h, group), half_of(half)].astype(jnp.float32)
            for half in range(2)
        ]
        for flow, (way, half, hops) in enumerate(flows):
            rcopy(stage, group, flow, hops - 1).wait_recv()
            halves[half] = halves[half] + slots[group, base[flow] + hops - 1].astype(jnp.float32)
        return jnp.concatenate(halves, axis=1)

    def spread(stage, group, step):
        for flow, (way, half, hops) in enumerate(flows):
            if 1 <= step <= hops:
                acopy(stage, group, flow, step - 1).wait_recv()
            if step < hops:
                acopy(stage, group, flow, step).start()

    def settled(with_gather=True):
        copy(slots, slots, rss.at[0], rsr.at[0, 0]).wait_send()
        if with_gather:
            copy(slots, slots, ags.at[0], agr.at[0, 0]).wait_send()

    def arrived(step):
        if step == 0:
            return [h]
        if step <= shorter:
            return [head(-step), head(step)]
        return [head(step)]

    def rows_at(step):
        return jnp.concatenate([x[share_rows(c), :] for c in arrived(step)], axis=0)

    def finish(stage, residual, events):
        for group in range(GROUPS):
            state_rows = pl.ds(group * piece, piece)
            total = summed(stage, group) + residual(group)
            state[state_rows, :] = total
            x[piece_rows(h, group), :] = normed(total)
            spread(stage, group, 0)
        events(0)
        for step in range(1, longer + 1):
            for group in range(GROUPS):
                spread(stage, group, step)
            events(step)
        settled()

    tile = min(256, rows)
    tiles = rows // tile

    def tile_rows(index, offset=0):
        return pl.ds(pl.multiple_of(offset + index * tile, tile), tile)

    def for_tiles(body):
        @pl.loop(0, tiles)
        def _(index):
            body(index)

    def norm_rows(src, dst):
        some = min(64, rows)

        @pl.loop(0, rows // some)
        def _(index):
            where = pl.ds(pl.multiple_of(index * some, some), some)
            dst[where, :] = normed(src[where, :].astype(jnp.float32))

    def project_q(stage, src):
        low = stages[stage][0]

        def body(index):
            q[tile_rows(index), :] = jnp.dot(
                src[tile_rows(index), :], wall[:, low : low + width], preferred_element_type=jnp.float32
            ).astype(jnp.bfloat16)

        for_tiles(body)

    def project_kv(stage, src, slab, offset):
        low = stages[stage][0]

        def body(index):
            slab[tile_rows(index, offset), :] = jnp.dot(
                src[tile_rows(index), :],
                wall[:, low + width : low + 3 * width],
                preferred_element_type=jnp.float32,
            ).astype(jnp.bfloat16)

        for_tiles(body)

    blocks = rows // BLOCK

    def block_at(i):
        farthest = lax.rem(h + nh // 2, nh) // (BLOCK // share)
        away = (i + 1) // 2 * (1 - 2 * lax.rem(i, 2)) * (1 - 2 * lax.rem(h, 2))
        return lax.rem(farthest + away + blocks, blocks)

    def attend(stage, index, slab, mask, keys, moving):
        lane = lax.broadcasted_iota(jnp.int32, (BLOCK, width), 1)
        where = pl.ds(pl.multiple_of(index * BLOCK, BLOCK), BLOCK)
        taken = pl.ds(pl.multiple_of(index * BLOCK, BLOCK), keys) if moving else pl.ds(0, keys)
        query = q[where, :]
        zero = jnp.zeros_like(query)
        both = jnp.concatenate(
            [jnp.where(lane < HD, query, zero), jnp.where(lane < HD, zero, query)], axis=0
        )
        scores = mask(contract_rows(both, slab[taken, 0:width]), index, where, taken)
        maxima = jnp.max(scores, axis=1, keepdims=True)
        expo = jnp.exp2((scores - maxima) * SCALE)
        totals = jnp.sum(expo, axis=1, keepdims=True)
        mixed = jnp.dot(
            expo.astype(jnp.bfloat16),
            slab[taken, width : 2 * width],
            preferred_element_type=jnp.float32,
        )
        mixed = mixed / totals
        mixed = jnp.where(lane < HD, mixed[:BLOCK], mixed[BLOCK:]).astype(jnp.bfloat16)
        low = stages[stage][0] + 3 * width
        p[stage % 2 if stage < 2 else 1, where, :] = contract_rows(
            mixed, wall[:, low : low + width]
        ).astype(jnp.bfloat16)

    def listed_mask(bias):
        def mask(scores, index, where, taken):
            return scores + bias[pl.ds(index, 1), :]

        return mask

    def window_mask(scores, index, where, taken):
        ids = query_ids[where, :]
        same = jnp.concatenate([ids, ids], axis=0) == key_ids[:, taken]
        return jnp.where(same, scores, NEGATIVE)

    def side(slab, o, first, where=None):
        k = 0 if o == 1 else 1
        start, count = (0, rows) if where is None else where
        return copy(
            slab.at[pl.ds(pl.multiple_of(rows + start, share), count), :],
            slab.at[pl.ds(pl.multiple_of((1 - o) * rows + start, share), count), :],
            hs.at[first + k],
            hr.at[first + k],
            band=band(o),
        )

    def fill_bias(lists, counts, bias):
        lane = lax.broadcasted_iota(jnp.int32, lists.shape, 1)
        slot = lax.broadcasted_iota(jnp.int32, (lists.shape[0], 1), 0).astype(jnp.float32)
        places = lax.broadcasted_iota(jnp.int32, (lists.shape[0], 3 * rows), 1)
        places = lax.shift_right_logical(places, BLOCK.bit_length() - 1).astype(jnp.float32)
        listed = lists[...].astype(jnp.float32)
        counted = counts[...].astype(jnp.float32)
        first = ((b - 1) * blocks).astype(jnp.float32)
        for index in range(blocks):
            mine = lane == b * blocks + index
            picked = jnp.sum(jnp.where(mine, listed, 0.0), axis=1, keepdims=True)
            count = jnp.sum(jnp.where(mine[:1], counted, 0.0), axis=1, keepdims=True)
            local = jnp.where(slot < count, picked - first, -1.0)
            hits = jnp.where(local == places, 0.0, NEGATIVE)
            bias[index : index + 1, :] = jnp.max(hits, axis=0, keepdims=True)

    def fill_ids():
        total = ids.shape[0]
        for k in range((2 * REACH + 1) * blocks):
            row = (b - REACH) * blocks + k
            inside = ((row >= 0) & (row < total)).astype(jnp.int32)
            found = ids[pl.ds(lax.rem(row + total, total), 1), :]
            key_ids[:, k * BLOCK : (k + 1) * BLOCK] = (found * inside + (inside - 1)).astype(
                jnp.float32
            )
        diagonal = lax.broadcasted_iota(jnp.int32, (BLOCK, BLOCK), 0) == lax.broadcasted_iota(
            jnp.int32, (BLOCK, BLOCK), 1
        )
        for k in range(blocks):
            row = key_ids[:, (REACH * blocks + k) * BLOCK : (REACH * blocks + k + 1) * BLOCK]
            query_ids[k * BLOCK : (k + 1) * BLOCK, :] = jnp.sum(
                jnp.where(diagonal, row, 0.0), axis=1, keepdims=True
            )

    zstart(0)
    zstart(1)
    norm_rows(mesh_ref, x)
    fill_bias(enc_list, enc_count, enc_bias)
    fill_bias(dec_list, dec_count, dec_bias)
    for step in range(1, z_steps + 1):
        zstep(0, step)
        if step == 1:
            norm_rows(grid_ref, gn)
            fill_ids()
        if step < z_steps:
            zstep(1, step)
    zfinish(0)
    project_kv(0, gn, eslab, rows)
    for o in (1, -1):
        side(eslab, o, 0).start()
    project_q(0, x)
    for o in (1, -1):
        side(eslab, o, 0).wait_recv()

    def encode(i):
        attend(0, block_at(i), eslab, listed_mask(enc_bias), 3 * rows, False)

    scattered(0, encode, ())
    zstep(1, z_steps)
    zfinish(1)

    def mesh_rows(group):
        return mesh_ref[piece_rows(h, group), :].astype(jnp.float32)

    def state_rows(group):
        return state[pl.ds(group * piece, piece), :]

    def part(place, where=None):
        start, count = (0, rows) if where is None else where
        return wslab.at[pl.ds(pl.multiple_of(place * rows + start, share), count), :]

    def window_moves(where=None):
        view = part(REACH, where)
        far = lax.rem(b + 6 * odd - 3 + nb, nb)
        return (
            copy(view, part(1, where), hs.at[2], hr.at[2], band=band(2)),
            copy(view, part(5, where), hs.at[3], hr.at[3], band=band(-2)),
            copy(view, part(6 - 6 * odd, where), hs.at[5], hr.at[5], band=far),
            copy(view, part(2 + 2 * odd, where), hs.at[4], hr.at[4], band=partner),
        )

    def proc_rows(step):
        low = stages[1][0]
        made = jnp.dot(
            rows_at(step), wall[:, low : low + 3 * width], preferred_element_type=jnp.float32
        ).astype(jnp.bfloat16)
        for k, chunk in enumerate(arrived(step)):
            mine = made[k * share : (k + 1) * share]
            q[share_rows(chunk), :] = mine[:, :width]
            wslab[share_rows(chunk, REACH * rows), :] = mine[:, width:]
            for move in window_moves((chunk * share, share)):
                move.start()

    finish(0, mesh_rows, proc_rows)

    zstart(2)
    moves = window_moves()
    passed = (
        copy(part(1), part(2 * odd), hs.at[6], hr.at[6], band=partner),
        copy(part(5), part(4 + 2 * odd), hs.at[7], hr.at[7], band=partner),
    )
    for move, onward in zip(moves, passed):
        move.wait_recv()
        onward.start()
    for move in (moves[3], moves[2], *passed):
        move.wait_recv()

    def process(i):
        attend(1, block_at(i), wslab, window_mask, 2 * REACH * rows + BLOCK, True)

    scattered(1, process, ((2, 1),))

    def after_processor(step):
        if step == 0:
            zstart(3)
        elif step % 2:
            zstep(2, longer // 2 + (step + 1) // 2)
        else:
            zstep(3, step // 2)

    finish(1, state_rows, after_processor)
    zfinish(2)

    def feed(i):
        low = stages[2][0]
        where = pl.ds(pl.multiple_of(block_at(i) * BLOCK, BLOCK), BLOCK)
        inner = jnp.dot(x[where, :], wall[:, low : low + ff], preferred_element_type=jnp.float32)
        hidden = (inner * 0.5 * (1.0 + lax.erf(inner * 0.5**0.5))).astype(jnp.bfloat16)
        p[0, where, :] = contract_rows(hidden, wall[:, low + ff : low + 2 * ff]).astype(jnp.bfloat16)

    scattered(2, feed, ((3, longer // 2 + 1),))
    zfinish(3)

    def dec_rows(step):
        low = stages[3][0]
        made = jnp.dot(
            rows_at(step), wall[:, low + width : low + 3 * width], preferred_element_type=jnp.float32
        ).astype(jnp.bfloat16)
        for k, chunk in enumerate(arrived(step)):
            dslab[share_rows(chunk, rows), :] = made[k * share : (k + 1) * share]
            for o in (1, -1):
                side(dslab, o, 8, (chunk * share, share)).start()

    finish(2, state_rows, dec_rows)

    project_q(3, gn)
    for o in (1, -1):
        side(dslab, o, 8).wait_recv()

    def decode(i):
        attend(3, block_at(i), dslab, listed_mask(dec_bias), 3 * rows, False)

    scattered(3, decode, ())
    for group in range(GROUPS):
        residual = grid_ref[piece_rows(h, group), :].astype(jnp.float32)
        out_ref[pl.ds(group * piece, piece), :] = (residual + summed(3, group)).astype(jnp.bfloat16)
    settled(False)
    for o in (1, -1):
        side(eslab, o, 0).wait_send()
        side(dslab, o, 8).wait_send()
    for move in (*moves, *passed):
        move.wait_send()
    for stage in range(4):
        zsettle(stage)


def per_device(
    nb,
    nh,
    grid_feats,
    mesh_feats,
    enc_in,
    enc_out,
    proc_in,
    proc_out,
    ff_up,
    ff_down,
    dec_in,
    dec_out,
    enc_list,
    enc_count,
    dec_list,
    dec_count,
    window_ids,
):
    rows, depth = mesh_feats.shape
    assert grid_feats.shape == mesh_feats.shape and WINDOW <= REACH * rows
    assert nh == rows // BLOCK * 2
    width = enc_in.shape[2]
    wrows, ff = ff_up.shape
    share = rows // nh
    nz = nb // 2
    blocks = rows // BLOCK
    given = (
        grid_feats,
        mesh_feats,
        enc_in,
        enc_out.T,
        proc_in,
        proc_out.T,
        ff_up,
        ff_down.T,
        dec_in,
        dec_out.T,
        enc_list.T,
        enc_count[None, :],
        dec_list.T,
        dec_count[None, :],
        window_ids.reshape(-1, BLOCK),
    )
    bf16, f32 = jnp.bfloat16, jnp.float32
    dma = pltpu.SemaphoreType.DMA
    msgs = 2 * (nh - 1)
    vmem = pl.BlockSpec(memory_space=pltpu.VMEM)
    return pl.pallas_call(
        functools.partial(kernel, nb, nh),
        out_shape=jax.ShapeDtypeStruct((share, depth), bf16),
        in_specs=[vmem] * len(given),
        out_specs=vmem,
        scratch_shapes=[
            pltpu.VMEM((nb * wrows, 12 * width + 2 * ff), bf16),
            pltpu.VMEM((rows, depth), bf16),
            pltpu.VMEM((rows, depth), bf16),
            pltpu.VMEM((rows, width), bf16),
            pltpu.VMEM((2, rows, depth), bf16),
            pltpu.VMEM((GROUPS, msgs, share // GROUPS, depth // 2), bf16),
            pltpu.VMEM((3 * rows, 2 * width), bf16),
            pltpu.VMEM(((2 * REACH + 1) * rows, 2 * width), bf16),
            pltpu.VMEM((3 * rows, 2 * width), bf16),
            pltpu.VMEM((share, depth), f32),
            pltpu.VMEM((blocks, 3 * rows), f32),
            pltpu.VMEM((blocks, 3 * rows), f32),
            pltpu.VMEM((1, (2 * REACH + 1) * rows), f32),
            pltpu.VMEM((rows, 1), f32),
            dma((4,)),
            dma((4, 2, 2, max(1, nz // 4))),
            dma((4,)),
            dma((1,)),
            dma((GROUPS, msgs)),
            dma((1,)),
            dma((GROUPS, msgs)),
            dma((10,)),
            dma((10,)),
        ],
        compiler_params=pltpu.CompilerParams(
            collective_id=0, has_side_effects=True, vmem_limit_bytes=60 * 1024 * 1024
        ),
    )(*given)


def solution(mesh):
    rows = P(("members", "band"), None)
    placed = (
        rows,
        rows,
        P(None, "band", "head"),
        P("head", "band"),
        P(None, "band", "head"),
        P("head", "band"),
        P("band", "head"),
        P("head", "band"),
        P(None, "band", "head"),
        P("head", "band"),
        P(),
        P(),
        P(),
        P(),
        P(),
    )
    return jax.shard_map(
        functools.partial(per_device, mesh.shape["band"], mesh.shape["head"]),
        mesh=mesh,
        in_specs=placed,
        out_specs=P(("members", "band", "head"), None),
        check_vma=False,
    )
```

```python
import functools

import jax
import jax.numpy as jnp
from jax import lax
from jax.experimental import pallas as pl
from jax.experimental.pallas import tpu as pltpu
from jax.sharding import PartitionSpec as P

HD = 64
BLOCK = 128
WINDOW = 1536
REACH = 3
GROUPS = 4
EPSILON = 1e-05
NEGATIVE = -1e30
SCALE = HD ** (-0.5) * 1.4426950408889634
MESH_ID = pl.DeviceIdType.MESH


def contract_rows(left, right):
    return lax.dot_general(left, right, (((1,), (1,)), ((), ())), preferred_element_type=jnp.float32)


def normed(values):
    centred = values - jnp.mean(values, axis=-1, keepdims=True)
    variance = jnp.mean(centred * centred, axis=-1, keepdims=True)
    return (centred * lax.rsqrt(variance + EPSILON)).astype(jnp.bfloat16)


def kernel(
    nb,
    nh,
    grid_ref,
    mesh_ref,
    enc_in,
    enc_out,
    proc_in,
    proc_out,
    ff_up,
    ff_down,
    dec_in,
    dec_out,
    enc_list,
    enc_count,
    dec_list,
    dec_count,
    ids,
    out_ref,
    wall,
    x,
    gn,
    q,
    p,
    slots,
    eslab,
    wslab,
    dslab,
    state,
    enc_bias,
    dec_bias,
    key_ids,
    query_ids,
    zs,
    zr,
    pr,
    rss,
    rsr,
    ags,
    agr,
    hs,
    hr,
):
    b = lax.axis_index("band")
    h = lax.axis_index("head")
    rows, depth = grid_ref.shape
    width = q.shape[1]
    ff = ff_up.shape[1]
    share = rows // nh
    half_cols = depth // 2
    wrows = ff_up.shape[0]
    nz = nb // 2
    odd = lax.rem(b, 2)
    partner = b + 1 - 2 * odd
    stages = (
        (0, 4 * width),
        (4 * width, 8 * width),
        (8 * width, 8 * width + 2 * ff),
        (8 * width + 2 * ff, 12 * width + 2 * ff),
    )

    def band(offset):
        return lax.rem(b + (offset + nb), nb)

    def head(offset):
        return lax.rem(h + (offset + nh), nh)

    def copy(src, dst, send_sem, recv_sem, **where):
        return pltpu.make_async_remote_copy(
            src_ref=src,
            dst_ref=dst,
            send_sem=send_sem,
            recv_sem=recv_sem,
            device_id={"band": where.get("band", b), "head": where.get("head", h)},
            device_id_type=MESH_ID,
        )

    place = 0
    own_rows = pl.ds(pl.multiple_of(b * wrows, wrows), wrows)
    for three, out in ((enc_in, enc_out), (proc_in, proc_out), (ff_up, ff_down), (dec_in, dec_out)):
        pieces = [three[k] for k in range(3)] if len(three.shape) == 3 else [three[...]]
        for one in (*pieces, out[...]):
            wall[own_rows, place : place + one.shape[1]] = one
            place += one.shape[1]

    barrier = pltpu.get_barrier_semaphore()
    peers = [{"band": band(o), "head": h} for o in (1, -1, 2, -2, 3, -3, 4, -4)]
    peers += [{"band": b, "head": head(o)} for o in (1, -1)]
    for peer in peers:
        pl.semaphore_signal(barrier, inc=1, device_id=peer, device_id_type=MESH_ID)
    pl.semaphore_wait(barrier, len(peers))

    reaches = (nz // 2, nz - 1 - nz // 2)
    z_steps = (reaches[0] + 1) // 2

    def wall_rows(start, count, stage):
        low, high = stages[stage]
        return wall.at[pl.ds(pl.multiple_of(start * wrows, wrows), count * wrows), low:high]

    def zcopy(stage, way, near, step):
        side_of = -1 if way else 1
        view = wall_rows(band(-4 * side_of * step), 1, stage)
        return copy(
            view,
            view,
            zs.at[stage],
            zr.at[stage, way, near, step],
            band=band(side_of * (2 if near else 4)),
        )

    def hand_over(stage, way, distance):
        view = wall_rows(band(2 * distance if way else -2 * distance), 1, stage)
        copy(view, view, zs.at[stage], pr.at[stage], band=partner).start()

    def zstart(stage):
        for way, reach in enumerate(reaches):
            if reach >= 2:
                zcopy(stage, way, 0, 0).start()
            if reach >= 1:
                zcopy(stage, way, 1, 0).start()
        hand_over(stage, 0, 0)

    def zstep(stage, step):
        if isinstance(step, int):
            when = lambda condition: (lambda body: body() if condition else None)
        else:
            when = pl.when
        for way, reach in enumerate(reaches):

            @when(2 * step <= reach)
            def _(way=way, reach=reach):
                zcopy(stage, way, 0, step - 1).wait_recv()

                @when(2 * step + 2 <= reach)
                def _():
                    zcopy(stage, way, 0, step).start()

                @when(2 * step + 1 <= reach)
                def _():
                    zcopy(stage, way, 1, step).start()

        for way, reach in enumerate(reaches):

            @when(2 * step <= reach)
            def _(way=way):
                hand_over(stage, way, 2 * step)

            @when(2 * step - 1 <= reach)
            def _(way=way):
                zcopy(stage, way, 1, step - 1).wait_recv()
                hand_over(stage, way, 2 * step - 1)

    def zfinish(stage):
        whole = wall_rows(0, nz, stage)
        copy(whole, whole, zs.at[stage], pr.at[stage]).wait_recv()

    def zsettle(stage):
        whole = wall_rows(0, 2 * nz - 1, stage)
        copy(whole, whole, zs.at[stage], pr.at[stage]).wait_send()

    longer = nh // 2
    shorter = nh - 1 - longer
    flows = ((1, 0, longer), (-1, 1, longer), (1, 1, shorter), (-1, 0, shorter))
    base = (0, longer, 2 * longer, 2 * longer + shorter)
    piece = share // GROUPS

    def share_rows(chunk, offset=0):
        return pl.ds(pl.multiple_of(offset + chunk * share, share), share)

    def piece_rows(chunk, group):
        return pl.ds(pl.multiple_of(chunk * share + group * piece, piece), piece)

    def half_of(half):
        return slice(half * half_cols, (half + 1) * half_cols)

    def rcopy(stage, group, flow, step):
        way, half, hops = flows[flow]
        slot = base[flow] + step
        return copy(
            p.at[stage % 2, piece_rows(head(way * (hops - step)), group), half_of(half)],
            slots.at[group, slot],
            rss.at[0],
            rsr.at[group, slot],
            head=head(way),
        )

    def acopy(stage, group, flow, step):
        way, half, hops = flows[flow]
        slot = base[flow] + step
        view = x.at[piece_rows(head(-way * step), group), half_of(half)]
        return copy(view, view, ags.at[0], agr.at[group, slot], head=head(way))

    def scattered(stage, produce, ticks):
        @pl.loop(0, longer + 1)
        def _(i):
            between = (i + longer - 1) // longer * ((2 * longer - 1 - i) // longer)

            @pl.loop(0, 1 + between)
            def _(side_of):
                produce(head((1 - 2 * side_of) * (longer - i)))

            @pl.when(i < longer)
            def _():
                pass_on(stage, i, ticks)

    def pass_on(stage, i, ticks):
        for group in range(GROUPS):
            for flow, (way, half, hops) in enumerate(flows):
                lag = longer - hops

                def go(group=group, flow=flow, way=way, half=half, hops=hops, lag=lag):
                    step = i - lag

                    @pl.when(step > 0)
                    def _():
                        rcopy(stage, group, flow, step - 1).wait_recv()
                        where = piece_rows(head(way * (hops - step)), group)
                        p[stage % 2, where, half_of(half)] = (
                            p[stage % 2, where, half_of(half)].astype(jnp.float32)
                            + slots[group, base[flow] + step - 1].astype(jnp.float32)
                        ).astype(jnp.bfloat16)

                    rcopy(stage, group, flow, step).start()

                if lag:
                    pl.when(i >= lag)(go)
                else:
                    go()
        for z_stage, first in ticks:

            @pl.when(lax.rem(i, 2) == 1)
            def _(z_stage=z_stage, first=first):
                zstep(z_stage, first + i // 2)

    def summed(stage, group):
        halves = [
            p[stage % 2, piece_rows(h, group), half_of(half)].astype(jnp.float32)
            for half in range(2)
        ]
        for flow, (way, half, hops) in enumerate(flows):
            rcopy(stage, group, flow, hops - 1).wait_recv()
            halves[half] = halves[half] + slots[group, base[flow] + hops - 1].astype(jnp.float32)
        return jnp.concatenate(halves, axis=1)

    def spread(stage, group, step):
        for flow, (way, half, hops) in enumerate(flows):
            if 1 <= step <= hops:
                acopy(stage, group, flow, step - 1).wait_recv()
            if step < hops:
                acopy(stage, group, flow, step).start()

    def settled(with_gather=True):
        copy(slots, slots, rss.at[0], rsr.at[0, 0]).wait_send()
        if with_gather:
            copy(slots, slots, ags.at[0], agr.at[0, 0]).wait_send()

    def arrived(step):
        if step == 0:
            return [h]
        if step <= shorter:
            return [head(-step), head(step)]
        return [head(step)]

    def rows_at(step):
        return jnp.concatenate([x[share_rows(c), :] for c in arrived(step)], axis=0)

    def finish(stage, residual, events):
        for group in range(GROUPS):
            state_rows = pl.ds(group * piece, piece)
            total = summed(stage, group) + residual(group)
            state[state_rows, :] = total
            x[piece_rows(h, group), :] = normed(total)
            spread(stage, group, 0)
        events(0)
        for step in range(1, longer + 1):
            for group in range(GROUPS):
                spread(stage, group, step)
            events(step)
        settled()

    tile = min(256, rows)
    tiles = rows // tile

    def tile_rows(index, offset=0):
        return pl.ds(pl.multiple_of(offset + index * tile, tile), tile)

    def for_tiles(body):
        @pl.loop(0, tiles)
        def _(index):
            body(index)

    def norm_rows(src, dst):
        some = min(64, rows)

        @pl.loop(0, rows // some)
        def _(index):
            where = pl.ds(pl.multiple_of(index * some, some), some)
            dst[where, :] = normed(src[where, :].astype(jnp.float32))

    def project_q(stage, src):
        low = stages[stage][0]

        def body(index):
            q[tile_rows(index), :] = jnp.dot(
                src[tile_rows(index), :], wall[:, low : low + width], preferred_element_type=jnp.float32
            ).astype(jnp.bfloat16)

        for_tiles(body)

    def project_kv(stage, src, slab, offset):
        low = stages[stage][0]

        def body(index):
            slab[tile_rows(index, offset), :] = jnp.dot(
                src[tile_rows(index), :],
                wall[:, low + width : low + 3 * width],
                preferred_element_type=jnp.float32,
            ).astype(jnp.bfloat16)

        for_tiles(body)

    blocks = rows // BLOCK

    def attend(stage, chunk, slab, mask, keys, moving):
        lane = lax.broadcasted_iota(jnp.int32, (share, width), 1)
        index = chunk // (BLOCK // share)
        where = share_rows(chunk)
        taken = pl.ds(pl.multiple_of(index * BLOCK, BLOCK), keys) if moving else pl.ds(0, keys)
        query = q[where, :]
        zero = jnp.zeros_like(query)
        both = jnp.concatenate(
            [jnp.where(lane < HD, query, zero), jnp.where(lane < HD, zero, query)], axis=0
        )
        scores = mask(contract_rows(both, slab[taken, 0:width]), index, where, taken)
        maxima = jnp.max(scores, axis=1, keepdims=True)
        expo = jnp.exp2((scores - maxima) * SCALE)
        totals = jnp.sum(expo, axis=1, keepdims=True)
        mixed = jnp.dot(
            expo.astype(jnp.bfloat16),
            slab[taken, width : 2 * width],
            preferred_element_type=jnp.float32,
        )
        mixed = mixed / totals
        mixed = jnp.where(lane < HD, mixed[:share], mixed[share:]).astype(jnp.bfloat16)
        low = stages[stage][0] + 3 * width
        p[stage % 2 if stage < 2 else 1, where, :] = contract_rows(
            mixed, wall[:, low : low + width]
        ).astype(jnp.bfloat16)

    def listed_mask(bias):
        def mask(scores, index, where, taken):
            return scores + bias[pl.ds(index, 1), :]

        return mask

    def window_mask(scores, index, where, taken):
        ids = query_ids[where, :]
        same = jnp.concatenate([ids, ids], axis=0) == key_ids[:, taken]
        return jnp.where(same, scores, NEGATIVE)

    def side(slab, o, first, where=None):
        k = 0 if o == 1 else 1
        start, count = (0, rows) if where is None else where
        return copy(
            slab.at[pl.ds(pl.multiple_of(rows + start, share), count), :],
            slab.at[pl.ds(pl.multiple_of((1 - o) * rows + start, share), count), :],
            hs.at[first + k],
            hr.at[first + k],
            band=band(o),
        )

    def fill_bias(lists, counts, bias):
        lane = lax.broadcasted_iota(jnp.int32, lists.shape, 1)
        slot = lax.broadcasted_iota(jnp.int32, (lists.shape[0], 1), 0).astype(jnp.float32)
        places = lax.broadcasted_iota(jnp.int32, (lists.shape[0], 3 * rows), 1)
        places = lax.shift_right_logical(places, BLOCK.bit_length() - 1).astype(jnp.float32)
        listed = lists[...].astype(jnp.float32)
        counted = counts[...].astype(jnp.float32)
        first = ((b - 1) * blocks).astype(jnp.float32)
        for index in range(blocks):
            mine = lane == b * blocks + index
            picked = jnp.sum(jnp.where(mine, listed, 0.0), axis=1, keepdims=True)
            count = jnp.sum(jnp.where(mine[:1], counted, 0.0), axis=1, keepdims=True)
            local = jnp.where(slot < count, picked - first, -1.0)
            hits = jnp.where(local == places, 0.0, NEGATIVE)
            bias[index : index + 1, :] = jnp.max(hits, axis=0, keepdims=True)

    def fill_ids():
        total = ids.shape[0]
        for k in range((2 * REACH + 1) * blocks):
            row = (b - REACH) * blocks + k
            inside = ((row >= 0) & (row < total)).astype(jnp.int32)
            found = ids[pl.ds(lax.rem(row + total, total), 1), :]
            key_ids[:, k * BLOCK : (k + 1) * BLOCK] = (found * inside + (inside - 1)).astype(
                jnp.float32
            )
        diagonal = lax.broadcasted_iota(jnp.int32, (BLOCK, BLOCK), 0) == lax.broadcasted_iota(
            jnp.int32, (BLOCK, BLOCK), 1
        )
        for k in range(blocks):
            row = key_ids[:, (REACH * blocks + k) * BLOCK : (REACH * blocks + k + 1) * BLOCK]
            query_ids[k * BLOCK : (k + 1) * BLOCK, :] = jnp.sum(
                jnp.where(diagonal, row, 0.0), axis=1, keepdims=True
            )

    zstart(0)
    zstart(1)
    norm_rows(mesh_ref, x)
    fill_bias(enc_list, enc_count, enc_bias)
    fill_bias(dec_list, dec_count, dec_bias)
    for step in range(1, z_steps + 1):
        zstep(0, step)
        if step == 1:
            norm_rows(grid_ref, gn)
            fill_ids()
        if step < z_steps:
            zstep(1, step)
    zfinish(0)
    project_kv(0, gn, eslab, rows)
    for o in (1, -1):
        side(eslab, o, 0).start()
    project_q(0, x)
    for o in (1, -1):
        side(eslab, o, 0).wait_recv()

    def encode(chunk):
        attend(0, chunk, eslab, listed_mask(enc_bias), 3 * rows, False)

    scattered(0, encode, ())
    zstep(1, z_steps)
    zfinish(1)

    def mesh_rows(group):
        return mesh_ref[piece_rows(h, group), :].astype(jnp.float32)

    def state_rows(group):
        return state[pl.ds(group * piece, piece), :]

    def part(place, where=None):
        start, count = (0, rows) if where is None else where
        return wslab.at[pl.ds(pl.multiple_of(place * rows + start, share), count), :]

    def window_moves(where=None):
        view = part(REACH, where)
        far = lax.rem(b + 6 * odd - 3 + nb, nb)
        return (
            copy(view, part(1, where), hs.at[2], hr.at[2], band=band(2)),
            copy(view, part(5, where), hs.at[3], hr.at[3], band=band(-2)),
            copy(view, part(6 - 6 * odd, where), hs.at[5], hr.at[5], band=far),
            copy(view, part(2 + 2 * odd, where), hs.at[4], hr.at[4], band=partner),
        )

    def proc_rows(step):
        low = stages[1][0]
        made = jnp.dot(
            rows_at(step), wall[:, low : low + 3 * width], preferred_element_type=jnp.float32
        ).astype(jnp.bfloat16)
        for k, chunk in enumerate(arrived(step)):
            mine = made[k * share : (k + 1) * share]
            q[share_rows(chunk), :] = mine[:, :width]
            wslab[share_rows(chunk, REACH * rows), :] = mine[:, width:]
            for move in window_moves((chunk * share, share)):
                move.start()

    finish(0, mesh_rows, proc_rows)

    zstart(2)
    moves = window_moves()
    passed = (
        copy(part(1), part(2 * odd), hs.at[6], hr.at[6], band=partner),
        copy(part(5), part(4 + 2 * odd), hs.at[7], hr.at[7], band=partner),
    )
    for move, onward in zip(moves, passed):
        move.wait_recv()
        onward.start()
    for move in (moves[3], moves[2], *passed):
        move.wait_recv()

    def process(chunk):
        attend(1, chunk, wslab, window_mask, 2 * REACH * rows + BLOCK, True)

    scattered(1, process, ((2, 1),))

    def after_processor(step):
        if step == 0:
            zstart(3)
        elif step % 2:
            zstep(2, longer // 2 + (step + 1) // 2)
        else:
            zstep(3, step // 2)

    finish(1, state_rows, after_processor)
    zfinish(2)

    def feed(chunk):
        low = stages[2][0]
        where = share_rows(chunk)
        inner = jnp.dot(x[where, :], wall[:, low : low + ff], preferred_element_type=jnp.float32)
        hidden = (inner * 0.5 * (1.0 + lax.erf(inner * 0.5**0.5))).astype(jnp.bfloat16)
        p[0, where, :] = contract_rows(hidden, wall[:, low + ff : low + 2 * ff]).astype(jnp.bfloat16)

    scattered(2, feed, ((3, longer // 2 + 1),))
    zfinish(3)

    def dec_rows(step):
        low = stages[3][0]
        made = jnp.dot(
            rows_at(step), wall[:, low + width : low + 3 * width], preferred_element_type=jnp.float32
        ).astype(jnp.bfloat16)
        for k, chunk in enumerate(arrived(step)):
            dslab[share_rows(chunk, rows), :] = made[k * share : (k + 1) * share]
            for o in (1, -1):
                side(dslab, o, 8, (chunk * share, share)).start()

    finish(2, state_rows, dec_rows)

    project_q(3, gn)
    for o in (1, -1):
        side(dslab, o, 8).wait_recv()

    def decode(chunk):
        attend(3, chunk, dslab, listed_mask(dec_bias), 3 * rows, False)

    scattered(3, decode, ())
    for group in range(GROUPS):
        residual = grid_ref[piece_rows(h, group), :].astype(jnp.float32)
        out_ref[pl.ds(group * piece, piece), :] = (residual + summed(3, group)).astype(jnp.bfloat16)
    settled(False)
    for o in (1, -1):
        side(eslab, o, 0).wait_send()
        side(dslab, o, 8).wait_send()
    for move in (*moves, *passed):
        move.wait_send()
    for stage in range(4):
        zsettle(stage)


def per_device(
    nb,
    nh,
    grid_feats,
    mesh_feats,
    enc_in,
    enc_out,
    proc_in,
    proc_out,
    ff_up,
    ff_down,
    dec_in,
    dec_out,
    enc_list,
    enc_count,
    dec_list,
    dec_count,
    window_ids,
):
    rows, depth = mesh_feats.shape
    assert grid_feats.shape == mesh_feats.shape and WINDOW <= REACH * rows
    assert nh == rows // BLOCK * 2
    width = enc_in.shape[2]
    wrows, ff = ff_up.shape
    share = rows // nh
    nz = nb // 2
    blocks = rows // BLOCK
    given = (
        grid_feats,
        mesh_feats,
        enc_in,
        enc_out.T,
        proc_in,
        proc_out.T,
        ff_up,
        ff_down.T,
        dec_in,
        dec_out.T,
        enc_list.T,
        enc_count[None, :],
        dec_list.T,
        dec_count[None, :],
        window_ids.reshape(-1, BLOCK),
    )
    bf16, f32 = jnp.bfloat16, jnp.float32
    dma = pltpu.SemaphoreType.DMA
    msgs = 2 * (nh - 1)
    vmem = pl.BlockSpec(memory_space=pltpu.VMEM)
    return pl.pallas_call(
        functools.partial(kernel, nb, nh),
        out_shape=jax.ShapeDtypeStruct((share, depth), bf16),
        in_specs=[vmem] * len(given),
        out_specs=vmem,
        scratch_shapes=[
            pltpu.VMEM((nb * wrows, 12 * width + 2 * ff), bf16),
            pltpu.VMEM((rows, depth), bf16),
            pltpu.VMEM((rows, depth), bf16),
            pltpu.VMEM((rows, width), bf16),
            pltpu.VMEM((2, rows, depth), bf16),
            pltpu.VMEM((GROUPS, msgs, share // GROUPS, depth // 2), bf16),
            pltpu.VMEM((3 * rows, 2 * width), bf16),
            pltpu.VMEM(((2 * REACH + 1) * rows, 2 * width), bf16),
            pltpu.VMEM((3 * rows, 2 * width), bf16),
            pltpu.VMEM((share, depth), f32),
            pltpu.VMEM((blocks, 3 * rows), f32),
            pltpu.VMEM((blocks, 3 * rows), f32),
            pltpu.VMEM((1, (2 * REACH + 1) * rows), f32),
            pltpu.VMEM((rows, 1), f32),
            dma((4,)),
            dma((4, 2, 2, max(1, nz // 4))),
            dma((4,)),
            dma((1,)),
            dma((GROUPS, msgs)),
            dma((1,)),
            dma((GROUPS, msgs)),
            dma((10,)),
            dma((10,)),
        ],
        compiler_params=pltpu.CompilerParams(
            collective_id=0, has_side_effects=True, vmem_limit_bytes=60 * 1024 * 1024
        ),
    )(*given)


def solution(mesh):
    rows = P(("members", "band"), None)
    placed = (
        rows,
        rows,
        P(None, "band", "head"),
        P("head", "band"),
        P(None, "band", "head"),
        P("head", "band"),
        P("band", "head"),
        P("head", "band"),
        P(None, "band", "head"),
        P("head", "band"),
        P(),
        P(),
        P(),
        P(),
        P(),
    )
    return jax.shard_map(
        functools.partial(per_device, mesh.shape["band"], mesh.shape["head"]),
        mesh=mesh,
        in_specs=placed,
        out_specs=P(("members", "band", "head"), None),
        check_vma=False,
    )
```
